128 devices in a mesh: dp: 16 (over z, x), mp: 8 (over y, core).
Axes of the slice: x: 4, y: 4, z: 4, core: 2. Of those that a mesh axis runs over, the one named last changes fastest.
Arguments:
- tokens: bfloat16 [256, 4096], P('dp'), may hold values from -6 to 6
- norm_gain: float32 [4096], replicated, may hold values from 0.5 to 1.5
- router: bfloat16 [4096, 8], replicated, may hold values from -0.09375 to 0.09375
- w_gate: bfloat16 [8, 4096, 14336], P('mp', None, 'dp'), may hold values from -0.09375 to 0.09375
- w_up: bfloat16 [8, 4096, 14336], P('mp', None, 'dp'), may hold values from -0.09375 to 0.09375
- w_down: bfloat16 [8, 14336, 4096], P('mp', 'dp'), may hold values from -0.046875 to 0.046875
- final_gain: float32 [4096], replicated, may hold values from 0.5 to 1.5
- routes: int32 [256, 2], replicated, may hold values from 0 to 7, all different within a row; in each aligned block of 16 rows (0 to 15, 16 to 31, ...) at most 8 rows name the same one
- steer_hidden: bfloat16 [2, 256, 1024], P(None, 'dp'), may hold values from -6 to 6
- steer_query: bfloat16 [2, 256, 1024], P(None, 'dp', 'mp'), may hold values from -200 to 200
- steer_cache: bfloat16 [2, 2, 256, 64, 1024], P(None, None, 'dp', None, 'mp'), may hold values from -6 to 6
- steer_new: bfloat16 [2, 2, 256, 1024], P(None, None, 'dp', 'mp'), may hold values from -6 to 6
- cache_len: int32 [256], P('dp'), may hold values from 1 to 64
- steer_out: bfloat16 [2, 1024, 1024], P(None, 'mp'), may hold values from -0.1875 to 0.1875
- steer_gain: float32 [2, 1024], replicated, may hold values from 0.5 to 1.5
- base_head: bfloat16 [4096, 16000], P(None, ('dp', 'mp')), may hold values from -0.09375 to 0.09375
- steer_head: bfloat16 [2, 1024, 16000], P(None, None, ('dp', 'mp')), may hold values from -0.1875 to 0.1875
- inv_temp: float32 [256], replicated, may hold values from 0.5 to 40
Outputs:
- log_probs: float32 [256, 16000], P(None, ('dp', 'mp'))
The draws below stay inside these ranges and needn't reach their ends.
Inputs may be any that keep to these rules, and one draw needn't show every extreme that they name: The two routes of a sequence differ; in every aligned block of 16 sequences (the sequences of one index of dp) no expert is named more than 8 times. Positions at and after cache_len[s] of sequence s's cache are unused.
All inputs are finite; a program needn't handle non-finite values.
Results may differ from the reference program's by a relative error of at most 0.00105.
Values may be sent and summed in bfloat16 or wider, within the bound.
A program may use at most 128 MiB of HBM per device.

```python
import math
import jax
import jax.numpy as jnp
import numpy as np
from jax import lax

D = 4096
FF = 14336
VOCAB = 16000
STEER_HEADS = 8
HEAD_DIM = 128
SEQ_DEV = 16
CACHE = 64
EXPERTS = 8
CAP = 8
SEQS = 256
STEER_W = 1024
N_DP = 16


def cache_keys(key):
    raw = jax.random.normal(jax.random.fold_in(key, 11), (2, SEQS, CACHE, STEER_W), jnp.float32)
    return jnp.clip(raw, -6.0, 6.0)


def draw_steer_cache(key, part):
    keys = cache_keys(key)
    values = jnp.clip(jax.random.normal(jax.random.fold_in(key, 12), (2, SEQS, CACHE, STEER_W), jnp.float32), -6.0, 6.0)
    return jnp.stack([keys, values], axis=1).astype(jnp.bfloat16)


def draw_steer_query(key, part):
    drawn = jnp.clip(jax.random.normal(jax.random.fold_in(key, 13), (2, SEQS, STEER_W), jnp.float32), -6.0, 6.0)
    return drawn.astype(jnp.bfloat16)


def draw_inv_temp(key, part):
    spread = jax.random.uniform(jax.random.fold_in(key, 21), (SEQS,), jnp.float32)
    temper = 0.5 * jnp.exp(spread * math.log(4.0))
    return temper


def with_ends(entries, stream_key, smallest, top_value):
    dims = entries.shape
    place = [jax.random.randint(jax.random.fold_in(stream_key, axis), (), 0, dims[axis]) for axis in range(len(dims))]
    entries = entries.at[tuple(place)].set(smallest)
    longest = dims.index(max(dims))
    place[longest] = (place[longest] + 1) % dims[longest]
    return entries.at[tuple(place)].set(top_value)


def levels(key, dims, split, low, high):
    def one(position, blocks):
        draws = jax.random.uniform(jax.random.fold_in(jax.random.fold_in(key, 6), position), (blocks,), jnp.float32, low / len(split), high / len(split))
        return jnp.repeat(jnp.exp(draws), dims[position] // blocks).reshape((-1,) + (1,) * (len(dims) - position - 1))

    level = one(*split[0])
    for cut in split[1:]:
        level = level * one(*cut)
    return level


def shared_out(key, own, number, rows, number_of, top, reach, lean):
    ranking = jax.random.permutation(key, number_of)
    heavy_load, ordinary = portions_of(number_of, rows * top, reach, lean, True), portions_of(number_of, rows * top, reach, lean, False)
    places = jnp.arange(number_of)

    def named(tallies, offset_by):
        used = int((tallies > 0).sum())
        fixed = max(1, used // 4)
        passed = fixed + (places - fixed + offset_by * (used - fixed)) % max(1, number_of - fixed)
        return jnp.zeros((number_of,), jnp.int32).at[ranking[jnp.where(places < fixed, places, passed)]].set(jnp.asarray(tallies, jnp.int32))

    tallies = jnp.where(number % 4 == 0, named(heavy_load, number // 4), named(ordinary, number - number // 4 - 1))
    mixed = jax.random.permutation(jax.random.fold_in(own, 3), number_of)
    giver, receiver = mixed[0:number_of // 2 * 2:2], mixed[1:number_of // 2 * 2:2]
    room = jnp.minimum(tallies[giver] - 1, reach - tallies[receiver]) // 2
    room = jnp.where((giver == ranking[0]) | (receiver == ranking[0]) | (tallies[receiver] == 0), 0, jnp.maximum(room, 0))
    passed = jax.random.randint(jax.random.fold_in(own, 4), (number_of // 2,), 0, 1 << 20) % (room + 1)
    tallies = tallies.at[giver].add(-passed).at[receiver].add(passed)
    labels = jnp.searchsorted(jnp.cumsum(tallies), jnp.arange(rows * top), side="right").astype(jnp.int32)
    grid = labels.reshape(top, rows).T
    grid = grid[jax.random.permutation(jax.random.fold_in(own, 1), rows)]
    offset_by = jax.random.randint(jax.random.fold_in(own, 2), (rows, 1), 0, top)
    return jnp.take_along_axis(grid, (jnp.arange(top)[None, :] + offset_by) % top, axis=1)


def portions_of(number_of, total, bound, lean, full):
    loads = [(1 << 20) // math.isqrt(grade ** lean) + 1 for grade in range(1, number_of + 1)]
    largest = bound if full else min(bound, max(-(-total // number_of), total * loads[0] // sum(loads)))
    least = 1 if total - largest >= number_of - 1 else 0
    counts, rest = [largest] + [least] * (number_of - 1), total - largest - least * (number_of - 1)
    while rest > 0:
        free = [i for i in range(1, number_of) if counts[i] < largest] or [i for i in range(1, number_of) if counts[i] < bound]
        pool, budget = sum([loads[i] for i in free]), rest
        for i in free:
            addition = min(bound - counts[i], max(1, budget * loads[i] // pool), rest)
            counts[i] = counts[i] + addition
            rest = rest - addition
    return np.array(counts)


def bell_draw(stream_key, shape, deviation, limit, split=(), kind=jnp.bfloat16):
    array = deviation * jax.random.normal(stream_key, shape, jnp.float32)
    if split:
        array = array * levels(stream_key, shape, split, -0.22, 0.18)
    return jnp.clip(array, -limit, limit).astype(kind)


def setup_inputs(seed: int = 0) -> dict:
    splits = jax.random.split(jax.random.key(seed), 19)
    tokens = bell_draw(splits[0], (SEQS, D), 1.0, 6.0, ((0, 16),))
    norm_gain = jnp.clip(1.0 + 0.1 * jax.random.normal(splits[1], (D,), jnp.float32), 0.5, 1.5)
    router = bell_draw(splits[2], (D, EXPERTS), D ** -0.5, 0.09375)
    w_gate = bell_draw(splits[3], (EXPERTS, D, FF), D ** -0.5, 0.09375, ((0, 8), (2, 16)))
    w_up = bell_draw(splits[4], (EXPERTS, D, FF), D ** -0.5, 0.09375, ((0, 8), (2, 16)))
    w_down = bell_draw(splits[5], (EXPERTS, FF, D), FF ** -0.5, 0.046875, ((0, 8), (1, 16)))
    final_gain = jnp.clip(1.0 + 0.1 * jax.random.normal(splits[6], (D,), jnp.float32), 0.5, 1.5)
    routes_keys = jax.random.split(jax.random.fold_in(splits[7], 1), SEQS // SEQ_DEV)
    routes_turns = jax.random.permutation(jax.random.fold_in(splits[7], 3), SEQS // SEQ_DEV)
    routes = jax.vmap(lambda own, number: shared_out(jax.random.fold_in(splits[7], 2), own, number, SEQ_DEV, EXPERTS, 2, CAP, 1))(routes_keys, routes_turns).reshape((SEQS, 2))
    steer_hidden = bell_draw(splits[8], (2, SEQS, STEER_W), 1.0, 6.0, ((1, 16),))
    steer_query = draw_steer_query(jax.random.fold_in(splits[18], 71), 0)
    steer_cache = draw_steer_cache(jax.random.fold_in(splits[18], 71), 0)
    steer_new = bell_draw(splits[11], (2, 2, SEQS, STEER_W), 1.0, 6.0, ((2, 16), (3, 8)))
    cache_len = with_ends(jax.random.randint(splits[12], (SEQS,), 1, CACHE + 1), jax.random.fold_in(splits[12], 1), 1, CACHE).astype(jnp.int32)
    steer_out = bell_draw(splits[13], (2, STEER_W, STEER_W), STEER_W ** -0.5, 0.1875, ((1, 8),))
    steer_gain = jnp.clip(1.0 + 0.1 * jax.random.normal(splits[14], (2, STEER_W), jnp.float32), 0.5, 1.5)
    base_head = bell_draw(splits[15], (D, VOCAB), D ** -0.5, 0.09375, ((1, 128),))
    steer_head = bell_draw(splits[16], (2, STEER_W, VOCAB), STEER_W ** -0.5, 0.1875, ((2, 128),))
    inv_temp = draw_inv_temp(jax.random.fold_in(splits[18], 71), 0)
    return {"tokens": tokens, "norm_gain": norm_gain, "router": router, "w_gate": w_gate, "w_up": w_up, "w_down": w_down, "final_gain": final_gain, "routes": routes, "steer_hidden": steer_hidden, "steer_query": steer_query, "steer_cache": steer_cache, "steer_new": steer_new, "cache_len": cache_len, "steer_out": steer_out, "steer_gain": steer_gain, "base_head": base_head, "steer_head": steer_head, "inv_temp": inv_temp}


steer_alpha = 2.0
norm_eps = 1e-05

def rms_scale(values, gain):
    mean_sq = lax.optimization_barrier(jnp.mean(values * values, axis=-1, keepdims=True))
    return values * lax.rsqrt(mean_sq + norm_eps) * gain

def route_gates(normed, router, chosen, n_experts):
    logits = jnp.dot(normed, router, preferred_element_type=jnp.float32)
    marks = (chosen[:, :, None] == jnp.arange(n_experts, dtype=jnp.int32)[None, None, :]).astype(logits.dtype)
    picked = lax.optimization_barrier(jnp.sum(logits[:, None, :] * marks, axis=2))
    first = 1.0 / (1.0 + jnp.exp(picked[:, 1] - picked[:, 0]))
    second = 1.0 / (1.0 + jnp.exp(picked[:, 0] - picked[:, 1]))
    return jnp.stack([first, second], axis=1)

def slot_tables(block_routes, block_gates, expert, capacity, n_experts):
    flat = block_routes.reshape(-1)
    marks = (flat[:, None] == jnp.arange(n_experts, dtype=jnp.int32)[None, :]).astype(jnp.int32)
    earlier = jnp.cumsum(marks, axis=0) - marks
    rank = lax.optimization_barrier(jnp.sum(earlier * marks, axis=1)).reshape(block_routes.shape)
    mine = block_routes == expert
    hits = (mine[:, :, None] & (rank[:, :, None] == jnp.arange(capacity, dtype=jnp.int32)[None, None, :])).astype(block_gates.dtype)
    select = jnp.transpose(lax.optimization_barrier(jnp.sum(hits, axis=1)))
    combine = lax.optimization_barrier(jnp.sum(hits * block_gates[:, :, None], axis=1))
    return (select, combine)

def reference(tokens, norm_gain, router, w_gate, w_up, w_down, final_gain, routes, steer_hidden, steer_query, steer_cache, steer_new, cache_len, steer_out, steer_gain, base_head, steer_head, inv_temp):
    resid = tokens.astype(jnp.float32)
    normed = rms_scale(resid, norm_gain).astype(jnp.bfloat16)
    gates = route_gates(normed, router, routes, EXPERTS)
    route_blocks = routes.reshape(N_DP, SEQ_DEV, 2)
    gate_blocks = gates.reshape(N_DP, SEQ_DEV, 2)
    normed_blocks = normed.astype(jnp.float32).reshape(N_DP, SEQ_DEV, D)

    def expert_step(running, inputs):
        expert, gate_mat, up_mat, down_mat = inputs
        select, combine = jax.vmap(lambda rr, gg: slot_tables(rr, gg, expert, CAP, EXPERTS))(route_blocks, gate_blocks)
        rows = jnp.einsum('jcs,jsd->jcd', select, normed_blocks, precision=lax.Precision.HIGHEST)
        rows = rows.astype(jnp.bfloat16).reshape(N_DP * CAP, D)
        gate_part = jnp.dot(rows, gate_mat, preferred_element_type=jnp.float32)
        up_part = jnp.dot(rows, up_mat, preferred_element_type=jnp.float32)
        hidden = (jax.nn.silu(gate_part) * up_part).astype(jnp.bfloat16)
        slot_out = jnp.dot(hidden, down_mat, preferred_element_type=jnp.float32).reshape(N_DP, CAP, D)
        added = jnp.einsum('jsc,jcd->jsd', combine, slot_out, precision=lax.Precision.HIGHEST)
        return (running + added, None)
    start_moe = jnp.zeros((N_DP, SEQ_DEV, D), jnp.float32)
    moe, _ = lax.scan(expert_step, start_moe, (jnp.arange(EXPERTS, dtype=jnp.int32), w_gate, w_up, w_down))
    base_state = resid + moe.reshape(SEQS, D)
    base_normed = rms_scale(base_state, final_gain).astype(jnp.bfloat16)
    scale = 1.0 / HEAD_DIM ** 0.5
    queries = steer_query.astype(jnp.float32).reshape(2, SEQS, STEER_HEADS, HEAD_DIM)
    keys = steer_cache[:, 0].astype(jnp.float32).reshape(2, SEQS, CACHE, STEER_HEADS, HEAD_DIM)
    values = steer_cache[:, 1].astype(jnp.float32).reshape(2, SEQS, CACHE, STEER_HEADS, HEAD_DIM)
    new_keys = steer_new[:, 0].astype(jnp.float32).reshape(2, SEQS, STEER_HEADS, HEAD_DIM)
    new_values = steer_new[:, 1].astype(jnp.float32).reshape(2, SEQS, STEER_HEADS, HEAD_DIM)
    scores = jnp.einsum('mshd,msphd->mshp', queries, keys) * scale
    new_score = lax.optimization_barrier(jnp.sum(queries * new_keys, axis=3)) * scale
    live = (jnp.arange(CACHE, dtype=jnp.int32)[None, :] < cache_len[:, None])[None, :, None, :]
    masked = jnp.where(live, scores, -1e+30)
    summit = jnp.maximum(lax.optimization_barrier(jnp.max(masked, axis=3)), new_score)
    expo = jnp.where(live, jnp.exp(masked - summit[..., None]), 0.0)
    new_expo = jnp.exp(new_score - summit)
    denom = lax.optimization_barrier(jnp.sum(expo, axis=3)) + new_expo
    weights = (expo / denom[..., None]).astype(jnp.bfloat16).astype(jnp.float32)
    new_weight = (new_expo / denom).astype(jnp.bfloat16).astype(jnp.float32)
    attended = jnp.einsum('mshp,msphd->mshd', weights, values) + new_weight[..., None] * new_values
    attended = attended.reshape(2, SEQS, STEER_W).astype(jnp.bfloat16)
    proj = jnp.einsum('msw,mwv->msv', attended.astype(jnp.float32), steer_out.astype(jnp.float32))
    steer_state = steer_hidden.astype(jnp.float32) + proj
    steer_normed = rms_scale(steer_state, steer_gain[:, None, :]).astype(jnp.bfloat16)
    base_logits = jnp.dot(base_normed, base_head, preferred_element_type=jnp.float32)
    plus = jnp.dot(steer_normed[0], steer_head[0], preferred_element_type=jnp.float32)
    minus = jnp.dot(steer_normed[1], steer_head[1], preferred_element_type=jnp.float32)
    combined = inv_temp[:, None] * (base_logits + steer_alpha * (plus - minus))
    peak_val = lax.optimization_barrier(jnp.max(combined, axis=1, keepdims=True))
    total = lax.optimization_barrier(jnp.sum(jnp.exp(combined - peak_val), axis=1, keepdims=True))
    return combined - peak_val - jnp.log(total)
```

```python
import functools
import math

import jax
import jax.numpy as jnp
from jax import lax
from jax.experimental import pallas as pl
from jax.experimental.pallas import tpu as pltpu
from jax.sharding import PartitionSpec as P

F32 = jnp.float32
BF16 = jnp.bfloat16
EPS = 1e-5
ALPHA = 2.0
HEAD_DIM = 128
NC = 4
WC = 4


def iota(shape, dim):
    return lax.broadcasted_iota(jnp.int32, shape, dim)


def eye(rows, cols):
    return iota((rows, cols), 0) == iota((rows, cols), 1)


def to_col(row, rows):
    n = row.shape[1]
    return jnp.sum(jnp.where(eye(rows, n), row, 0.0), axis=1, keepdims=True)


def to_row(col, cols):
    n = col.shape[0]
    return jnp.sum(jnp.where(eye(n, cols), col, 0.0), axis=0, keepdims=True)


def nt(a, b):
    return lax.dot_general(a, b, (((1,), (1,)), ((), ())), preferred_element_type=F32)


def mm(a, b):
    return jnp.dot(a, b, preferred_element_type=F32)


def kernel(
    tokens_h, norm_gain_h, router_h, w_gate_h, w_up_h, w_down_h, final_gain_h, routes_h,
    hidden_h, query_h, cache_h, new_h, len_h, sout_h, sgain_h, bhead_h, shead_h, temp_h,
    out_ref,
    tokens, norm_gain, router, w_gate, w_up, w_down, final_gain, routes,
    hidden, query, cache, new, clen, sout, sgain, bhead, shead, temp,
    xs, xr, act, pbuf, prec, stbuf, sall, rsend, rrecv, msend, mrecv,
    xa, xb, sq1, sq2, sqs, lsend, l1, l2, slog, comb_s,
    lsem, bsem_s, bsem_r,
):
    dp = lax.axis_index("dp")
    mp = lax.axis_index("mp")
    y, c = mp // 2, mp % 2
    z, x = dp // 4, dp % 4

    dp_peers = [
        (lax.rem(z + k // 4, 4) * 4 + lax.rem(x + k % 4, 4), mp)
        for k in (1, 3, 4, 12, 5, 7, 13, 15, 2, 8, 6, 14, 9, 11, 10)
    ]
    dp_slot = (1, 3, 4, 12, 5, 7, 13, 15, 2, 8, 6, 14, 9, 11, 10)
    def dp_from(k):
        return (lax.rem(z + 4 - k // 4, 4) * 4 + lax.rem(x + 4 - k % 4, 4), mp)

    mp_peers = [(dp, lax.rem(mp + k, 8)) for k in range(1, 8)]
    y_peers = [(dp, lax.rem(y + k, 4) * 2 + c) for k in (1, 3, 2)]
    sibling = (dp, y * 2 + 1 - c)

    def rcopy(src, dst, phase, dev):
        return pltpu.make_async_remote_copy(
            src_ref=src, dst_ref=dst, send_sem=bsem_s.at[phase], recv_sem=bsem_r.at[phase],
            device_id=dev, device_id_type=pl.DeviceIdType.MESH,
        )

    pending = []

    def send(src, dst, phase, dev):
        rcopy(src, dst, phase, dev).start()

    def wait_in(ref, phase):
        rcopy(ref, ref, phase, sibling).wait_recv()

    def sent(ref, phase):
        pending.append((ref, phase))

    (X, PR, ST, S1, S2, S3, M, A1, A2, A3, B1, B2, B3, Q1, Q2, L1, L2) = range(17)
    R0 = 17

    pairs = [
        (tokens_h, tokens), (norm_gain_h, norm_gain), (routes_h, routes), (router_h, router),
        (query_h, query), (cache_h, cache), (new_h, new), (len_h, clen), (sout_h, sout),
        (hidden_h, hidden), (sgain_h, sgain),
        (final_gain_h, final_gain), (temp_h, temp),
    ]
    late = [(w_down_h.at[0], w_down), (shead_h, shead), (bhead_h, bhead)]
    copies = {}

    def fetch(src, dst, n):
        cp = pltpu.make_async_copy(src, dst, lsem.at[n])
        cp.start()
        return cp

    n = 0
    for src, dst in pairs:
        copies[id(dst)] = fetch(src, dst, n)
        n += 1
    barrier = pltpu.get_barrier_semaphore()
    for dev in dp_peers + mp_peers:
        pl.semaphore_signal(barrier, inc=1, device_id=dev, device_id_type=pl.DeviceIdType.MESH)
    wcopies = []
    kw = w_gate.shape[0] // WC
    for i in range(WC):
        rows = pl.ds(i * kw, kw)
        wcopies.append(fetch(w_gate_h.at[0, rows], w_gate.at[rows], n))
        wcopies.append(fetch(w_up_h.at[0, rows], w_up.at[rows], n + 1))
        n += 2
    for src, dst in late:
        copies[id(dst)] = fetch(src, dst, n)
        n += 1

    def need(*refs):
        for r in refs:
            copies[id(r)].wait()

    need(tokens, norm_gain, routes)
    tok = tokens[...].astype(F32)
    mean_sq = jnp.mean(tok * tok, axis=1, keepdims=True)
    normed = (tok * lax.rsqrt(mean_sq + EPS) * norm_gain[...]).astype(BF16)
    rt = routes[...]
    lanes = iota((16, 256), 1)
    own = lanes == dp * 16 + iota((16, 256), 0)
    earlier = (lanes >= dp * 16) & (lanes < dp * 16 + iota((16, 256), 0))
    rt0, rt1 = rt[0:1, :], rt[1:2, :]
    hit_all = ((rt0 == mp) | (rt1 == mp)).astype(F32)
    r0 = jnp.sum(jnp.where(own, rt0.astype(F32), 0.0), axis=1, keepdims=True)
    r1 = jnp.sum(jnp.where(own, rt1.astype(F32), 0.0), axis=1, keepdims=True)
    hit = jnp.sum(jnp.where(own, hit_all, 0.0), axis=1, keepdims=True)
    rank = jnp.sum(jnp.where(earlier, hit_all, 0.0), axis=1, keepdims=True)
    hit_row = jnp.sum(jnp.where(eye(16, 128), hit, 0.0), axis=0, keepdims=True)
    rank_row = jnp.sum(
        jnp.where(iota((16, 128), 0) < iota((16, 128), 1), hit, 0.0), axis=0, keepdims=True
    )
    select = jnp.where(
        (hit_row > 0.5) & (rank_row == iota((8, 128), 0).astype(F32)), 1.0, 0.0
    )[:, :16].astype(BF16)
    slot_in = mm(select, normed).astype(BF16)
    xs[...] = slot_in
    xr[0] = slot_in

    pl.semaphore_wait(barrier, 22)
    for k, dev in zip(dp_slot, dp_peers):
        send(xs, xr.at[k], X, dev)
    sent(xr.at[pl.ds(0, 15)], X)

    need(query, cache, new, clen, sout)
    len_col = to_col(clen[...].astype(F32), 16).astype(jnp.int32)
    pos = iota((16, 1024), 1) - 64 * iota((16, 1024), 0)
    live = (pos >= 0) & (pos < len_col)
    scale = 1.0 / math.sqrt(HEAD_DIM)
    for m in range(2):
        q = query[m]
        scores = nt(q, cache[m, 0].reshape(1024, 128)) * scale
        new_score = (
            jnp.sum(q.astype(F32) * new[m, 0].astype(F32), axis=1, keepdims=True) * scale
        )
        masked = jnp.where(live, scores, -1e30)
        summit = jnp.maximum(jnp.max(masked, axis=1, keepdims=True), new_score)
        expo = jnp.where(live, jnp.exp(masked - summit), 0.0)
        new_expo = jnp.exp(new_score - summit)
        denom = jnp.sum(expo, axis=1, keepdims=True) + new_expo
        weights = (expo / denom).astype(BF16)
        new_weight = (new_expo / denom).astype(BF16).astype(F32)
        att = mm(weights, cache[m, 1].reshape(1024, 128)) + new_weight * new[m, 1].astype(F32)
        proj = mm(att.astype(BF16), sout[m])
        for e in range(8):
            pbuf[e, m] = proj[:, e * 128 : (e + 1) * 128]
    for k, dev in enumerate(mp_peers):
        send(pbuf.at[dev[1]], prec.at[k], PR, dev)
    sent(prec, PR)

    need(router)
    logits = nt(normed, router[...])
    experts = iota((16, 8), 1).astype(F32)
    p0 = jnp.sum(jnp.where(experts == r0, logits, 0.0), axis=1, keepdims=True)
    p1 = jnp.sum(jnp.where(experts == r1, logits, 0.0), axis=1, keepdims=True)
    mine = mp.astype(F32)
    gate = jnp.where(
        r0 == mine,
        1.0 / (1.0 + jnp.exp(p1 - p0)),
        jnp.where(r1 == mine, 1.0 / (1.0 + jnp.exp(p0 - p1)), 0.0),
    )
    comb_s[...] = jnp.where(
        (hit > 0.5) & (rank == iota((16, 128), 1).astype(F32)), gate, 0.0
    )

    need(hidden, sgain)
    wait_in(prec, PR)
    head_cols = pl.ds(pl.multiple_of(mp * 128, 128), 128)
    state = hidden[:, :, head_cols].astype(F32) + pbuf[mp]
    for k in range(7):
        state = state + prec[k]
    stbuf[mp] = state
    for dev in mp_peers:
        send(stbuf.at[mp], stbuf.at[mp], ST, dev)
    sent(stbuf.at[pl.ds(0, 7)], ST)
    wait_in(stbuf.at[pl.ds(0, 7)], ST)
    sq_sum = jnp.zeros((16, 1), F32)
    for e in range(8):
        part = stbuf[e, c]
        sq_sum = sq_sum + jnp.sum(part * part, axis=1, keepdims=True)
    inv = lax.rsqrt(sq_sum * (1.0 / 1024.0) + EPS)
    for h in range(2):
        cols = pl.ds(pl.multiple_of(y * 256 + h * 128, 128), 128)
        both = sgain[:, cols]
        g = jnp.where(c == 0, both[0:1], both[1:2])
        sall[c, y, dp, :, h * 128 : (h + 1) * 128] = (stbuf[2 * y + h, c] * inv * g).astype(BF16)
    for dev in dp_peers:
        send(sall.at[c, y, dp], sall.at[c, y, dp], S1, dev)
    sent(sall.at[0, 0, pl.ds(0, 15)], S1)

    wait_in(xr.at[pl.ds(1, 15)], X)
    for cp in wcopies:
        cp.wait()
    kx = xr.shape[2]

    def up_tile(col, width):
        rows = xr[...].reshape(128, kx)
        g = mm(rows, w_gate[:, pl.ds(col, width)])
        u = mm(rows, w_up[:, pl.ds(col, width)])
        act[:, pl.ds(col, width)] = (g / (1.0 + jnp.exp(-g)) * u).astype(BF16)

    ff = w_gate.shape[1]
    full = ff // 256

    def up_body(i, carry):
        up_tile(pl.multiple_of(i * 256, 256), 256)
        return carry

    lax.fori_loop(0, full, up_body, 0)
    if ff % 256:
        up_tile(full * 256, ff % 256)

    wait_in(sall.at[0, 0, pl.ds(0, 15)], S1)
    for dev in y_peers:
        send(sall.at[c, y], sall.at[c, y], S2, dev)
    sent(sall.at[0, pl.ds(0, 3)], S2)

    need(w_down)
    wn = w_down.shape[1] // NC
    for q in range(NC):
        def down_body(i, carry):
            col = pl.multiple_of(q * wn + i * 256, 256)
            res = mm(act[...], w_down[:, pl.ds(col, 256)])
            rsend[q, :, :, pl.ds(pl.multiple_of(i * 256, 256), 256)] = res.reshape(
                16, 8, 256
            ).astype(BF16)
            return carry

        lax.fori_loop(0, wn // 256, down_body, 0)
        for k in dp_slot:
            send(rsend.at[q, k], rrecv.at[q, k], R0 + q, dp_from(k))
        sent(rsend.at[q, pl.ds(0, 15)], R0 + q)

    wait_in(sall.at[0, pl.ds(0, 3)], S2)
    send(sall.at[c], sall.at[c], S3, sibling)
    sent(sall.at[0], S3)
    need(shead)
    wait_in(sall.at[0], S3)
    for m in range(2):
        acc = None
        for yy in range(4):
            part = mm(sall[m, yy].reshape(256, 256), shead[m, yy * 256 : (yy + 1) * 256, :])
            acc = part if acc is None else acc + part
        if m == 0:
            slog[...] = acc
        else:
            slog[...] = ALPHA * (slog[...] - acc)

    comb = comb_s[...]
    for q in range(NC):
        wait_in(rrecv.at[q, pl.ds(1, 15)], R0 + q)
        total = rsend[q, 0].astype(F32)
        for k in range(1, 16):
            total = total + rrecv[q, k].astype(F32)
        mixed = None
        for s in range(8):
            term = comb[:, s : s + 1] * total[s : s + 1, :]
            mixed = term if mixed is None else mixed + term
        mixed = mixed.astype(BF16)
        per = wn // 512
        for h in range(per):
            msend[q * per + h] = mixed[:, h * 512 : (h + 1) * 512]
    for k, dev in enumerate(mp_peers):
        send(msend.at[dev[1]], mrecv.at[k], M, dev)
    sent(mrecv, M)
    need(final_gain)
    mine_cols = pl.ds(pl.multiple_of(mp * 512, 512), 512)
    state = tokens[:, mine_cols].astype(F32) + msend[mp].astype(F32)
    wait_in(mrecv, M)
    for k in range(7):
        state = state + mrecv[k].astype(F32)
    u = (state * final_gain[:, mine_cols]).astype(BF16)
    xa[c, dp, y] = u[:, 0:256]
    xb[c, y, dp] = u[:, 256:512]
    for dev in y_peers:
        send(xa.at[c, dp, y], xa.at[c, dp, y], A1, dev)
    sent(xa.at[0, 0, pl.ds(0, 3)], A1)
    for dev in dp_peers:
        send(xb.at[c, y, dp], xb.at[c, y, dp], B1, dev)
    sent(xb.at[0, 0, pl.ds(0, 15)], B1)
    part = to_row(jnp.sum(state * state, axis=1, keepdims=True), 128)
    sqs[...] = jnp.broadcast_to(part, (8, 128))
    for k, dev in enumerate(mp_peers):
        send(sqs, sq1.at[k], Q1, dev)
    sent(sq1, Q1)
    wait_in(xa.at[0, 0, pl.ds(0, 3)], A1)
    for dev in dp_peers:
        send(xa.at[c, dp], xa.at[c, dp], A2, dev)
    sent(xa.at[0, pl.ds(0, 15)], A2)
    wait_in(sq1, Q1)
    total = sqs[...]
    for k in range(7):
        total = total + sq1[k]
    sq2[dp] = total
    for dev in dp_peers:
        send(sq2.at[dp], sq2.at[dp], Q2, dev)
    sent(sq2.at[pl.ds(0, 15)], Q2)
    wait_in(xb.at[0, 0, pl.ds(0, 15)], B1)
    for dev in y_peers:
        send(xb.at[c, y], xb.at[c, y], B2, dev)
    sent(xb.at[0, pl.ds(0, 3)], B2)
    need(temp, bhead)
    temp_col = to_col(temp[...], 256)
    wait_in(sq2.at[pl.ds(0, 15)], Q2)
    sums = sq2[:, 0:1, :]
    sums = jnp.sum(
        jnp.where((iota((16, 16, 128), 1) == iota((16, 16, 128), 2)), sums, 0.0),
        axis=2, keepdims=True,
    ).reshape(256, 1)
    row_scale = lax.rsqrt(sums * (1.0 / 4096.0) + EPS)

    wait_in(xa.at[0, pl.ds(0, 15)], A2)
    send(xa.at[c], xa.at[c], A3, sibling)
    sent(xa.at[0], A3)

    def head_a(cc, acc):
        for yy in range(4):
            rows = pl.ds(pl.multiple_of((2 * yy + cc) * 512, 256), 256)
            part = mm(xa[cc, :, yy].reshape(256, 256), bhead[rows, :])
            acc = part if acc is None else acc + part
        return acc

    def head_b(cc, acc):
        for yy in range(4):
            rows = pl.ds(pl.multiple_of((2 * yy + cc) * 512 + 256, 256), 256)
            acc = acc + mm(xb[cc, yy].reshape(256, 256), bhead[rows, :])
        return acc

    acc = head_a(c, None)
    wait_in(xb.at[0, pl.ds(0, 3)], B2)
    send(xb.at[c], xb.at[c], B3, sibling)
    sent(xb.at[0], B3)
    acc = head_b(c, acc)
    wait_in(xa.at[0], A3)
    acc = head_a(1 - c, acc)
    wait_in(xb.at[0], B3)
    acc = head_b(1 - c, acc)

    combined = temp_col * (acc * row_scale + slog[...])
    peak = jnp.max(combined, axis=1, keepdims=True)
    total = jnp.sum(jnp.exp(combined - peak), axis=1, keepdims=True)
    lsend[0, 0:1] = to_row(peak, 256)
    lsend[0, 1:2] = to_row(total, 256)

    def merge(pk, tt, buf, count):
        top = pk
        for k in range(count):
            top = jnp.maximum(top, buf[k, 0:1])
        out = tt * jnp.exp(pk - top)
        for k in range(count):
            out = out + buf[k, 1:2] * jnp.exp(buf[k, 0:1] - top)
        return top, out

    for k, dev in enumerate(dp_peers):
        send(lsend.at[0], l1.at[k], L1, dev)
    sent(l1, L1)
    wait_in(l1, L1)
    pk, tt = merge(lsend[0, 0:1], lsend[0, 1:2], l1, 15)
    lsend[1, 0:1] = pk
    lsend[1, 1:2] = tt
    for k, dev in enumerate(mp_peers):
        send(lsend.at[1], l2.at[k], L2, dev)
    sent(l2, L2)
    wait_in(l2, L2)
    pk, tt = merge(pk, tt, l2, 7)
    out_ref[...] = combined - to_col(pk, 256) - to_col(jnp.log(tt), 256)

    for ref, phase in pending:
        rcopy(ref, ref, phase, sibling).wait_send()


def per_device(
    tokens, norm_gain, router, w_gate, w_up, w_down, final_gain, routes, steer_hidden,
    steer_query, steer_cache, steer_new, cache_len, steer_out, steer_gain, base_head,
    steer_head, inv_temp,
):
    args = (
        tokens, norm_gain.reshape(1, -1), router.T, w_gate, w_up, w_down,
        final_gain.reshape(1, -1), routes.T, steer_hidden, steer_query, steer_cache, steer_new,
        cache_len.reshape(1, -1), steer_out, steer_gain, base_head, steer_head,
        inv_temp.reshape(1, -1),
    )
    d = tokens.shape[1]
    vs = base_head.shape[1]

    def like(a, drop=0):
        return pltpu.VMEM(a.shape[drop:], a.dtype)

    fetched = [like(a, 1 if k in (3, 4, 5) else 0) for k, a in enumerate(args)]
    scratch = fetched + [
        pltpu.VMEM((8, d), BF16),
        pltpu.VMEM((16, 8, d), BF16),
        pltpu.VMEM((128, w_gate.shape[2]), BF16),
        pltpu.VMEM((8, 2, 16, 128), F32),
        pltpu.VMEM((7, 2, 16, 128), F32),
        pltpu.VMEM((8, 2, 16, 128), F32),
        pltpu.VMEM((2, 4, 16, 16, 256), BF16),
        pltpu.VMEM((NC, 16, 8, d // NC), BF16),
        pltpu.VMEM((NC, 16, 8, d // NC), BF16),
        pltpu.VMEM((8, 16, 512), BF16),
        pltpu.VMEM((7, 16, 512), BF16),
        pltpu.VMEM((2, 16, 4, 16, 256), BF16),
        pltpu.VMEM((2, 4, 16, 16, 256), BF16),
        pltpu.VMEM((7, 8, 128), F32),
        pltpu.VMEM((16, 8, 128), F32),
        pltpu.VMEM((8, 128), F32),
        pltpu.VMEM((2, 2, 256), F32),
        pltpu.VMEM((15, 2, 256), F32),
        pltpu.VMEM((7, 2, 256), F32),
        pltpu.VMEM((256, vs), F32),
        pltpu.VMEM((16, 128), F32),
        pltpu.SemaphoreType.DMA((13 + 2 * WC + 3,)),
        pltpu.SemaphoreType.DMA((17 + NC,)),
        pltpu.SemaphoreType.DMA((17 + NC,)),
    ]
    return pl.pallas_call(
        kernel,
        name="decode_step",
        out_shape=jax.ShapeDtypeStruct((256, vs), F32),
        in_specs=[pl.BlockSpec(memory_space=pl.ANY)] * len(args),
        out_specs=pl.BlockSpec(memory_space=pltpu.VMEM),
        scratch_shapes=scratch,
        compiler_params=pltpu.CompilerParams(
            collective_id=0, has_side_effects=True, vmem_limit_bytes=60 * 1024 * 1024
        ),
    )(*args)


def solution(mesh):
    placed = (
        P("dp", None),
        P(),
        P(),
        P("mp", None, "dp"),
        P("mp", None, "dp"),
        P("mp", "dp", None),
        P(),
        P(),
        P(None, "dp", None),
        P(None, "dp", "mp"),
        P(None, None, "dp", None, "mp"),
        P(None, None, "dp", "mp"),
        P("dp"),
        P(None, "mp", None),
        P(),
        P(None, ("dp", "mp")),
        P(None, None, ("dp", "mp")),
        P(),
    )
    return jax.shard_map(
        per_device, mesh=mesh, in_specs=placed, out_specs=P(None, ("dp", "mp")), check_vma=False
    )
```

```python
import functools
import math

import jax
import jax.numpy as jnp
from jax import lax
from jax.experimental import pallas as pl
from jax.experimental.pallas import tpu as pltpu
from jax.sharding import PartitionSpec as P

F32 = jnp.float32
BF16 = jnp.bfloat16
EPS = 1e-5
ALPHA = 2.0
HEAD_DIM = 128
WC = 4


def iota(shape, dim):
    return lax.broadcasted_iota(jnp.int32, shape, dim)


def eye(rows, cols):
    return iota((rows, cols), 0) == iota((rows, cols), 1)


def to_col(row, rows):
    n = row.shape[1]
    return jnp.sum(jnp.where(eye(rows, n), row, 0.0), axis=1, keepdims=True)


def to_row(col, cols):
    n = col.shape[0]
    return jnp.sum(jnp.where(eye(n, cols), col, 0.0), axis=0, keepdims=True)


def nt(a, b):
    return lax.dot_general(a, b, (((1,), (1,)), ((), ())), preferred_element_type=F32)


def mm(a, b):
    return jnp.dot(a, b, preferred_element_type=F32)


def kernel(
    tokens_h, norm_gain_h, router_h, w_gate_h, w_up_h, w_down_h, final_gain_h, routes_h,
    hidden_h, query_h, cache_h, new_h, len_h, sout_h, sgain_h, bhead_h, shead_h, temp_h,
    out_ref,
    tokens, norm_gain, router, w_gate, w_up, w_down, final_gain, routes,
    hidden, query, cache, new, clen, sout, sgain, bhead, shead, temp,
    xr, act, pbuf, prec, stbuf, sall, rsend, rrecv,
    xa, xb, sq1, sq2, sqs, lsend, l1, l2, slog, combs,
    lsem, bsem_s, bsem_r,
):
    dp = lax.axis_index("dp")
    mp = lax.axis_index("mp")
    y, c = mp // 2, mp % 2
    z, x = dp // 4, dp % 4

    zs = [z] + [lax.rem(z + k, 4) for k in (1, 2, 3)]
    xs = [x] + [lax.rem(x + k, 4) for k in (1, 2, 3)]

    def dp_at(kz, kx):
        return zs[kz % 4] * 4 + xs[kx % 4]

    dp_peers = [
        (dp_at(k // 4, k % 4), mp) for k in (1, 3, 4, 12, 5, 7, 13, 15, 2, 8, 6, 14, 9, 11, 10)
    ]
    mp_peers = [(dp, lax.rem(mp + k, 8)) for k in range(1, 8)]
    y_peers = [(dp, lax.rem(y + k, 4) * 2 + c) for k in (1, 3, 2)]
    sibling = (dp, y * 2 + 1 - c)

    def rcopy(src, dst, phase, dev):
        return pltpu.make_async_remote_copy(
            src_ref=src, dst_ref=dst, send_sem=bsem_s.at[phase], recv_sem=bsem_r.at[phase],
            device_id=dev, device_id_type=pl.DeviceIdType.MESH,
        )

    pending = []

    def send(src, dst, phase, dev):
        rcopy(src, dst, phase, dev).start()

    def wait_in(ref, phase):
        with jax.named_scope("wait%d" % phase):
            rcopy(ref, ref, phase, sibling).wait_recv()

    def sent(ref, phase):
        pending.append((ref, phase))

    (XA, XB, PR, ST, S1, S2, S3, A1, A2, A3, B1, B2, B3, Q1, Q2, L1, L2) = range(17)
    X1 = 16
    R0 = 23

    pairs = [
        (tokens_h, tokens), (norm_gain_h, norm_gain), (routes_h, routes), (router_h, router),
        (query_h, query), (cache_h, cache), (new_h, new), (len_h, clen), (sout_h, sout),
        (hidden_h, hidden), (sgain_h, sgain),
        (final_gain_h, final_gain), (temp_h, temp),
    ]
    late = [(w_down_h.at[0], w_down), (shead_h, shead), (bhead_h, bhead)]
    copies = {}

    def fetch(src, dst, n):
        cp = pltpu.make_async_copy(src, dst, lsem.at[n])
        cp.start()
        return cp

    n = 0
    for src, dst in pairs:
        copies[id(dst)] = fetch(src, dst, n)
        n += 1
    barrier = pltpu.get_barrier_semaphore()
    for dev in dp_peers + mp_peers:
        pl.semaphore_signal(barrier, inc=1, device_id=dev, device_id_type=pl.DeviceIdType.MESH)
    wcopies = []
    kw = w_gate.shape[0] // WC
    for i in range(WC):
        rows = pl.ds(i * kw, kw)
        wcopies.append(fetch(w_gate_h.at[0, rows], w_gate.at[rows], n))
        wcopies.append(fetch(w_up_h.at[0, rows], w_up.at[rows], n + 1))
        n += 2
    for src, dst in late:
        copies[id(dst)] = fetch(src, dst, n)
        n += 1

    def need(*refs):
        with jax.named_scope("need"):
            for r in refs:
                copies[id(r)].wait()

    need(tokens, norm_gain, routes)
    tok = tokens[...].astype(F32)
    mean_sq = jnp.mean(tok * tok, axis=1, keepdims=True)
    normed = (tok * lax.rsqrt(mean_sq + EPS) * norm_gain[...]).astype(BF16)
    rt = routes[...]
    lanes = iota((16, 256), 1)
    own = lanes == dp * 16 + iota((16, 256), 0)
    earlier = (lanes >= dp * 16) & (lanes < dp * 16 + iota((16, 256), 0))
    rt0, rt1 = rt[0:1, :], rt[1:2, :]

    def places(expert):
        hit_all = ((rt0 == expert) | (rt1 == expert)).astype(F32)
        hit = jnp.sum(jnp.where(own, hit_all, 0.0), axis=1, keepdims=True)
        rank = jnp.sum(jnp.where(earlier, hit_all, 0.0), axis=1, keepdims=True)
        return hit, rank

    hit, _ = places(mp)
    hit_row = jnp.sum(jnp.where(eye(16, 128), hit, 0.0), axis=0, keepdims=True)
    rank_row = jnp.sum(
        jnp.where(iota((16, 128), 0) < iota((16, 128), 1), hit, 0.0), axis=0, keepdims=True
    )
    select = jnp.where(
        (hit_row > 0.5) & (rank_row == iota((8, 128), 0).astype(F32)), 1.0, 0.0
    )[:, :16].astype(BF16)
    half = xr.shape[3]
    xr[0, 0] = mm(select, normed[:, :half]).astype(BF16)
    xr[1, 0] = mm(select, normed[:, half:]).astype(BF16)

    with jax.named_scope("barrier"):
        pl.semaphore_wait(barrier, 22)

    def to_x(kx):
        return (dp_at(0, kx), mp)

    def to_z(kz):
        return (dp_at(kz, 0), mp)

    for k in (1, 3, 2):
        send(xr.at[0, 0], xr.at[0, k], X1 + k, to_x(k))
        send(xr.at[1, 0], xr.at[1, 4 * k], X1 + 3 + k, to_z(k))
    for k in (1, 3, 2):
        send(xr.at[0, 0], xr.at[0, 4 * k], XA, to_z(k))
        send(xr.at[1, 0], xr.at[1, k], XB, to_x(k))

    def forward(k):
        wait_in(xr.at[0, k], X1 + k)
        for kz in (1, 3, 2):
            send(xr.at[0, k], xr.at[0, 4 * kz + k], XA, to_z(kz))
        wait_in(xr.at[1, 4 * k], X1 + 3 + k)
        for kx in (1, 3, 2):
            send(xr.at[1, 4 * k], xr.at[1, 4 * k + kx], XB, to_x(kx))
        sent(xr.at[0, 0], X1 + k)
        sent(xr.at[0, 0], X1 + 3 + k)

    sent(xr.at[0, pl.ds(0, 12)], XA)
    sent(xr.at[1, pl.ds(0, 12)], XB)

    need(query, cache, new, clen, sout)
    len_col = to_col(clen[...].astype(F32), 16).astype(jnp.int32)
    pos = iota((16, 1024), 1) - 64 * iota((16, 1024), 0)
    live = (pos >= 0) & (pos < len_col)
    scale = 1.0 / math.sqrt(HEAD_DIM)
    for m in range(2):
        q = query[m]
        scores = nt(q, cache[m, 0].reshape(1024, 128)) * scale
        new_score = (
            jnp.sum(q.astype(F32) * new[m, 0].astype(F32), axis=1, keepdims=True) * scale
        )
        masked = jnp.where(live, scores, -1e30)
        summit = jnp.maximum(jnp.max(masked, axis=1, keepdims=True), new_score)
        expo = jnp.where(live, jnp.exp(masked - summit), 0.0)
        new_expo = jnp.exp(new_score - summit)
        denom = jnp.sum(expo, axis=1, keepdims=True) + new_expo
        weights = (expo / denom).astype(BF16)
        new_weight = (new_expo / denom).astype(BF16).astype(F32)
        att = mm(weights, cache[m, 1].reshape(1024, 128)) + new_weight * new[m, 1].astype(F32)
        proj = mm(att.astype(BF16), sout[m])
        for e in range(8):
            pbuf[e, m] = proj[:, e * 128 : (e + 1) * 128]
    for k, dev in enumerate(mp_peers):
        send(pbuf.at[dev[1]], prec.at[k], PR, dev)
    sent(prec, PR)

    for k in (1, 3, 2):
        forward(k)

    need(router)
    logits = nt(normed, router[...])
    experts = iota((16, 8), 1).astype(F32)
    r0 = jnp.sum(jnp.where(own, rt0.astype(F32), 0.0), axis=1, keepdims=True)
    r1 = jnp.sum(jnp.where(own, rt1.astype(F32), 0.0), axis=1, keepdims=True)
    p0 = jnp.sum(jnp.where(experts == r0, logits, 0.0), axis=1, keepdims=True)
    p1 = jnp.sum(jnp.where(experts == r1, logits, 0.0), axis=1, keepdims=True)
    gate0 = 1.0 / (1.0 + jnp.exp(p1 - p0))
    gate1 = 1.0 / (1.0 + jnp.exp(p0 - p1))
    for i in range(8):
        expert = lax.rem(mp + 8 - i, 8)
        named = expert.astype(F32)
        _, rank = places(expert)
        gate = jnp.where(r0 == named, gate0, 0.0) + jnp.where(r1 == named, gate1, 0.0)
        combs[i] = jnp.where(rank == iota((16, 128), 1).astype(F32), gate, 0.0)

    need(hidden, sgain)
    wait_in(prec, PR)
    head_cols = pl.ds(pl.multiple_of(mp * 128, 128), 128)
    state = hidden[:, :, head_cols].astype(F32) + pbuf[mp]
    for k in range(7):
        state = state + prec[k]
    stbuf[mp] = state
    for dev in mp_peers:
        send(stbuf.at[mp], stbuf.at[mp], ST, dev)
    sent(stbuf.at[pl.ds(0, 7)], ST)
    wait_in(stbuf.at[pl.ds(0, 7)], ST)
    sq_sum = jnp.zeros((16, 1), F32)
    for e in range(8):
        part = stbuf[e, c]
        sq_sum = sq_sum + jnp.sum(part * part, axis=1, keepdims=True)
    inv = lax.rsqrt(sq_sum * (1.0 / 1024.0) + EPS)
    both = sgain[...]
    g = jnp.where(c == 0, both[0:1], both[1:2])
    for e in range(8):
        cols = slice(e * 128, (e + 1) * 128)
        sall[c, dp, :, cols] = (stbuf[e, c] * inv * g[:, cols]).astype(BF16)
    for dev in dp_peers:
        send(sall.at[c, dp], sall.at[c, dp], S1, dev)
    sent(sall.at[0, pl.ds(0, 15)], S1)

    wait_in(xr.at[0, pl.ds(0, 12)], XA)
    wait_in(xr.at[1, pl.ds(0, 12)], XB)
    with jax.named_scope("weights"):
        for cp in wcopies:
            cp.wait()

    def up_tile(col, width):
        cols = pl.ds(col, width)
        lo, hi = xr[0].reshape(128, half), xr[1].reshape(128, half)
        g = mm(lo, w_gate[:half, cols]) + mm(hi, w_gate[half:, cols])
        u = mm(lo, w_up[:half, cols]) + mm(hi, w_up[half:, cols])
        act[:, pl.ds(col, width)] = (g / (1.0 + jnp.exp(-g)) * u).astype(BF16)

    ff = w_gate.shape[1]
    full = ff // 256

    def up_body(i, carry):
        up_tile(pl.multiple_of(i * 256, 256), 256)
        return carry

    lax.fori_loop(0, full, up_body, 0)
    if ff % 256:
        up_tile(full * 256, ff % 256)

    need(w_down)
    wn = rsend.shape[3]
    for i in range(8):
        owner = lax.rem(mp + i, 8)
        for h in range(wn // 256):
            col = pl.multiple_of(owner * wn + h * 256, 256)
            res = mm(act[...], w_down[:, pl.ds(col, 256)])
            rsend[i, :, :, h * 256 : (h + 1) * 256] = res.reshape(16, 8, 256).astype(BF16)
        for k in range(0 if i else 1, 16):
            send(
                rsend.at[i, k], rrecv.at[i, k], R0 + i,
                (dp_at(4 - k // 4, 4 - k % 4), owner),
            )
        sent(rsend.at[i, pl.ds(0, 16 if i else 15)], R0 + i)

    wait_in(sall.at[0, pl.ds(0, 15)], S1)
    send(sall.at[c], sall.at[c], S3, sibling)
    sent(sall.at[0], S3)
    need(shead)
    wait_in(sall.at[0], S3)
    slog[...] = ALPHA * (
        nt(sall[0].reshape(256, 1024), shead[:, 0, :])
        - nt(sall[1].reshape(256, 1024), shead[:, 1, :])
    )

    need(final_gain)
    mine_cols = pl.ds(pl.multiple_of(mp * wn, wn), wn)
    state = tokens[:, mine_cols].astype(F32)
    for i in range(8):
        if i:
            wait_in(rrecv.at[i], R0 + i)
            total = rrecv[i, 0].astype(F32)
        else:
            wait_in(rrecv.at[i, pl.ds(1, 15)], R0 + i)
            total = rsend[i, 0].astype(F32)
        for k in range(1, 16):
            total = total + rrecv[i, k].astype(F32)
        comb = combs[i]
        for s in range(8):
            state = state + comb[:, s : s + 1] * total[s : s + 1, :]
    u = (state * final_gain[:, mine_cols]).astype(BF16)
    xa[c, dp, y] = u[:, 0:256]
    xb[c, y, dp] = u[:, 256:512]
    for dev in y_peers:
        send(xa.at[c, dp, y], xa.at[c, dp, y], A1, dev)
    sent(xa.at[0, 0, pl.ds(0, 3)], A1)
    for dev in dp_peers:
        send(xb.at[c, y, dp], xb.at[c, y, dp], B1, dev)
    sent(xb.at[0, 0, pl.ds(0, 15)], B1)
    part = to_row(jnp.sum(state * state, axis=1, keepdims=True), 128)
    sqs[...] = jnp.broadcast_to(part, (8, 128))
    for k, dev in enumerate(mp_peers):
        send(sqs, sq1.at[k], Q1, dev)
    sent(sq1, Q1)
    wait_in(xa.at[0, 0, pl.ds(0, 3)], A1)
    for dev in dp_peers:
        send(xa.at[c, dp], xa.at[c, dp], A2, dev)
    sent(xa.at[0, pl.ds(0, 15)], A2)
    wait_in(sq1, Q1)
    total = sqs[...]
    for k in range(7):
        total = total + sq1[k]
    sq2[dp] = total
    for dev in dp_peers:
        send(sq2.at[dp], sq2.at[dp], Q2, dev)
    sent(sq2.at[pl.ds(0, 15)], Q2)
    wait_in(xb.at[0, 0, pl.ds(0, 15)], B1)
    for dev in y_peers:
        send(xb.at[c, y], xb.at[c, y], B2, dev)
    sent(xb.at[0, pl.ds(0, 3)], B2)
    need(temp, bhead)
    temp_col = to_col(temp[...], 256)
    wait_in(xa.at[0, pl.ds(0, 15)], A2)
    send(xa.at[c], xa.at[c], A3, sibling)
    sent(xa.at[0], A3)
    wait_in(sq2.at[pl.ds(0, 15)], Q2)
    sums = sq2[:, 0:1, :]
    sums = jnp.sum(
        jnp.where((iota((16, 16, 128), 1) == iota((16, 16, 128), 2)), sums, 0.0),
        axis=2, keepdims=True,
    ).reshape(256, 1)
    row_scale = lax.rsqrt(sums * (1.0 / 4096.0) + EPS)


    def head_a(cc, acc):
        for yy in range(4):
            rows = pl.ds(pl.multiple_of((2 * yy + cc) * 512, 256), 256)
            part = mm(xa[cc, :, yy].reshape(256, 256), bhead[rows, :])
            acc = part if acc is None else acc + part
        return acc

    def head_b(cc, acc):
        for yy in range(4):
            rows = pl.ds(pl.multiple_of((2 * yy + cc) * 512 + 256, 256), 256)
            acc = acc + mm(xb[cc, yy].reshape(256, 256), bhead[rows, :])
        return acc

    acc = head_a(c, None)
    wait_in(xb.at[0, pl.ds(0, 3)], B2)
    send(xb.at[c], xb.at[c], B3, sibling)
    sent(xb.at[0], B3)
    acc = head_b(c, acc)
    wait_in(xa.at[0], A3)
    acc = head_a(1 - c, acc)
    wait_in(xb.at[0], B3)
    acc = head_b(1 - c, acc)

    combined = temp_col * (acc * row_scale + slog[...])
    peak = jnp.max(combined, axis=1, keepdims=True)
    lse = peak + jnp.log(jnp.sum(jnp.exp(combined - peak), axis=1, keepdims=True))

    def merge(first, buf, count):
        top = first
        for k in range(count):
            top = jnp.maximum(top, buf[k])
        out = jnp.exp(first - top)
        for k in range(count):
            out = out + jnp.exp(buf[k] - top)
        return top + jnp.log(out)

    row = to_row(lse, 256)
    lsend[0] = row
    for k, dev in enumerate(dp_peers):
        send(lsend.at[0], l1.at[k], L1, dev)
    sent(l1, L1)
    wait_in(l1, L1)
    row = merge(row, l1, 15)
    lsend[1] = row
    for k, dev in enumerate(mp_peers):
        send(lsend.at[1], l2.at[k], L2, dev)
    sent(l2, L2)
    wait_in(l2, L2)
    out_ref[...] = combined - to_col(merge(row, l2, 7), 256)

    for ref, phase in pending:
        rcopy(ref, ref, phase, sibling).wait_send()


def per_device(
    tokens, norm_gain, router, w_gate, w_up, w_down, final_gain, routes, steer_hidden,
    steer_query, steer_cache, steer_new, cache_len, steer_out, steer_gain, base_head,
    steer_head, inv_temp,
):
    args = (
        tokens, norm_gain.reshape(1, -1), router.T, w_gate, w_up, w_down,
        final_gain.reshape(1, -1), routes.T, steer_hidden, steer_query, steer_cache, steer_new,
        cache_len.reshape(1, -1), steer_out, steer_gain, base_head,
        jnp.transpose(steer_head, (2, 0, 1)), inv_temp.reshape(1, -1),
    )
    d = tokens.shape[1]
    vs = base_head.shape[1]

    def like(a, drop=0):
        return pltpu.VMEM(a.shape[drop:], a.dtype)

    fetched = [like(a, 1 if k in (3, 4, 5) else 0) for k, a in enumerate(args)]
    scratch = fetched + [
        pltpu.VMEM((2, 16, 8, d // 2), BF16),
        pltpu.VMEM((128, w_gate.shape[2]), BF16),
        pltpu.VMEM((8, 2, 16, 128), F32),
        pltpu.VMEM((7, 2, 16, 128), F32),
        pltpu.VMEM((8, 2, 16, 128), F32),
        pltpu.VMEM((2, 16, 16, 1024), BF16),
        pltpu.VMEM((8, 16, 8, d // 8), BF16),
        pltpu.VMEM((8, 16, 8, d // 8), BF16),
        pltpu.VMEM((2, 16, 4, 16, 256), BF16),
        pltpu.VMEM((2, 4, 16, 16, 256), BF16),
        pltpu.VMEM((7, 8, 128), F32),
        pltpu.VMEM((16, 8, 128), F32),
        pltpu.VMEM((8, 128), F32),
        pltpu.VMEM((2, 1, 256), F32),
        pltpu.VMEM((15, 1, 256), F32),
        pltpu.VMEM((7, 1, 256), F32),
        pltpu.VMEM((256, vs), F32),
        pltpu.VMEM((8, 16, 128), F32),
        pltpu.SemaphoreType.DMA((13 + 2 * WC + 3,)),
        pltpu.SemaphoreType.DMA((31,)),
        pltpu.SemaphoreType.DMA((31,)),
    ]
    return pl.pallas_call(
        kernel,
        name="decode_step",
        out_shape=jax.ShapeDtypeStruct((256, vs), F32),
        in_specs=[pl.BlockSpec(memory_space=pltpu.HBM)] * len(args),
        out_specs=pl.BlockSpec(memory_space=pltpu.VMEM),
        scratch_shapes=scratch,
        compiler_params=pltpu.CompilerParams(
            collective_id=0, has_side_effects=True, vmem_limit_bytes=44 * 1024 * 1024
        ),
    )(*[pltpu.with_memory_space_constraint(a, pltpu.HBM) for a in args])


def solution(mesh):
    placed = (
        P("dp", None),
        P(),
        P(),
        P("mp", None, "dp"),
        P("mp", None, "dp"),
        P("mp", "dp", None),
        P(),
        P(),
        P(None, "dp", None),
        P(None, "dp", "mp"),
        P(None, None, "dp", None, "mp"),
        P(None, None, "dp", "mp"),
        P("dp"),
        P(None, "mp", None),
        P(),
        P(None, ("dp", "mp")),
        P(None, None, ("dp", "mp")),
        P(),
    )
    return jax.shard_map(
        per_device, mesh=mesh, in_specs=placed, out_specs=P(None, ("dp", "mp")), check_vma=False
    )
```

```python
import functools
import math

import jax
import jax.numpy as jnp
from jax import lax
from jax.experimental import pallas as pl
from jax.experimental.pallas import tpu as pltpu
from jax.sharding import PartitionSpec as P

F32 = jnp.float32
BF16 = jnp.bfloat16
EPS = 1e-5
ALPHA = 2.0
HEAD_DIM = 128
WC = 4


def iota(shape, dim):
    return lax.broadcasted_iota(jnp.int32, shape, dim)


def eye(rows, cols):
    return iota((rows, cols), 0) == iota((rows, cols), 1)


def to_col(row, rows):
    n = row.shape[1]
    return jnp.sum(jnp.where(eye(rows, n), row, 0.0), axis=1, keepdims=True)


def to_row(col, cols):
    n = col.shape[0]
    return jnp.sum(jnp.where(eye(n, cols), col, 0.0), axis=0, keepdims=True)


def nt(a, b):
    return lax.dot_general(a, b, (((1,), (1,)), ((), ())), preferred_element_type=F32)


def mm(a, b):
    return jnp.dot(a, b, preferred_element_type=F32)


def kernel(
    tokens_h, norm_gain_h, router_h, w_gate_h, w_up_h, w_down_h, final_gain_h, routes_h,
    hidden_h, query_h, cache_h, new_h, len_h, sout_h, sgain_h, bhead_h, shead_h, temp_h,
    out_ref,
    tokens, norm_gain, router, w_gate, w_up, w_down, final_gain, routes,
    hidden, query, cache, new, clen, sout, sgain, bhead, shead, temp,
    xr, act, pbuf, prec, stbuf, sall, r1s, r1r, r2s, r2r, m1s, m1r, d2s, d2r, gs, gr, wh, wl,
    xa, xb, bhs, psib, prcv, pown, sq1, sq2, sqs, lsend, l1, l2, slog, comb_s,
    lsem, bsem_s, bsem_r,
):
    dp = lax.axis_index("dp")
    mp = lax.axis_index("mp")
    y, c = mp // 2, mp % 2
    z, x = dp // 4, dp % 4

    zs = [z] + [lax.rem(z + k, 4) for k in (1, 2, 3)]
    xs = [x] + [lax.rem(x + k, 4) for k in (1, 2, 3)]

    def dp_at(kz, kx):
        return zs[kz % 4] * 4 + xs[kx % 4]

    dp_peers = [
        (dp_at(k // 4, k % 4), mp) for k in (1, 3, 4, 12, 5, 7, 13, 15, 2, 8, 6, 14, 9, 11, 10)
    ]
    mp_peers = [(dp, lax.rem(mp + k, 8)) for k in range(1, 8)]
    y_peers = [(dp, lax.rem(y + k, 4) * 2 + c) for k in (1, 3, 2)]
    sibling = (dp, y * 2 + 1 - c)

    def rcopy(src, dst, phase, dev):
        return pltpu.make_async_remote_copy(
            src_ref=src, dst_ref=dst, send_sem=bsem_s.at[phase], recv_sem=bsem_r.at[phase],
            device_id=dev, device_id_type=pl.DeviceIdType.MESH,
        )

    pending = []

    def send(src, dst, phase, dev):
        rcopy(src, dst, phase, dev).start()

    def wait_in(ref, phase):
        with jax.named_scope("wait%d" % phase):
            rcopy(ref, ref, phase, sibling).wait_recv()

    def sent(ref, phase):
        pending.append((ref, phase))

    (XA, XB, PR, ST, SA, SB, S3, A2, B1, B2, HD, PX, Q1, Q2, L1, L2, G, M1, D2, R2, R1) = range(21)
    X1, Y1 = 21, 27

    pairs = [
        (tokens_h, tokens), (norm_gain_h, norm_gain), (routes_h, routes), (router_h, router),
        (query_h, query), (cache_h, cache), (new_h, new), (len_h, clen), (sout_h, sout),
        (hidden_h, hidden), (sgain_h, sgain),
        (final_gain_h, final_gain), (temp_h, temp),
    ]
    late = [(w_down_h.at[0], w_down), (shead_h, shead), (bhead_h, bhead)]
    copies = {}

    def fetch(src, dst, n):
        cp = pltpu.make_async_copy(src, dst, lsem.at[n])
        cp.start()
        return cp

    n = 0
    for src, dst in pairs:
        copies[id(dst)] = fetch(src, dst, n)
        n += 1
    barrier = pltpu.get_barrier_semaphore()
    for dev in dp_peers + mp_peers:
        pl.semaphore_signal(barrier, inc=1, device_id=dev, device_id_type=pl.DeviceIdType.MESH)
    wcopies = []
    kw = w_gate.shape[0] // WC
    for i in range(WC):
        rows = pl.ds(i * kw, kw)
        wcopies.append(fetch(w_gate_h.at[0, rows], w_gate.at[rows], n))
        wcopies.append(fetch(w_up_h.at[0, rows], w_up.at[rows], n + 1))
        n += 2
    for src, dst in late:
        copies[id(dst)] = fetch(src, dst, n)
        n += 1

    def need(*refs):
        with jax.named_scope("need"):
            for r in refs:
                copies[id(r)].wait()

    need(tokens, norm_gain, routes)
    tok = tokens[...].astype(F32)
    mean_sq = jnp.mean(tok * tok, axis=1, keepdims=True)
    normed = (tok * lax.rsqrt(mean_sq + EPS) * norm_gain[...]).astype(BF16)
    rt = routes[...]
    lanes = iota((16, 256), 1)
    own = lanes == dp * 16 + iota((16, 256), 0)
    earlier = (lanes >= dp * 16) & (lanes < dp * 16 + iota((16, 256), 0))
    rt0, rt1 = rt[0:1, :], rt[1:2, :]

    def places(expert):
        hit_all = ((rt0 == expert) | (rt1 == expert)).astype(F32)
        hit = jnp.sum(jnp.where(own, hit_all, 0.0), axis=1, keepdims=True)
        rank = jnp.sum(jnp.where(earlier, hit_all, 0.0), axis=1, keepdims=True)
        return hit, rank

    hit, rank = places(mp)
    hit_row = jnp.sum(jnp.where(eye(16, 128), hit, 0.0), axis=0, keepdims=True)
    rank_row = jnp.sum(
        jnp.where(iota((16, 128), 0) < iota((16, 128), 1), hit, 0.0), axis=0, keepdims=True
    )
    select = jnp.where(
        (hit_row > 0.5) & (rank_row == iota((8, 128), 0).astype(F32)), 1.0, 0.0
    )[:, :16].astype(BF16)
    half = xr.shape[3]
    xr[0, 0] = mm(select, normed[:, :half]).astype(BF16)
    xr[1, 0] = mm(select, normed[:, half:]).astype(BF16)

    need(query, cache, new, clen, sout)
    len_col = to_col(clen[...].astype(F32), 16).astype(jnp.int32)
    pos = iota((16, 1024), 1) - 64 * iota((16, 1024), 0)
    live = (pos >= 0) & (pos < len_col)
    scale = 1.0 / math.sqrt(HEAD_DIM)
    for m in range(2):
        q = query[m]
        scores = nt(q, cache[m, 0].reshape(1024, 128)) * scale
        new_score = (
            jnp.sum(q.astype(F32) * new[m, 0].astype(F32), axis=1, keepdims=True) * scale
        )
        masked = jnp.where(live, scores, -1e30)
        summit = jnp.maximum(jnp.max(masked, axis=1, keepdims=True), new_score)
        expo = jnp.where(live, jnp.exp(masked - summit), 0.0)
        new_expo = jnp.exp(new_score - summit)
        denom = jnp.sum(expo, axis=1, keepdims=True) + new_expo
        weights = (expo / denom).astype(BF16)
        new_weight = (new_expo / denom).astype(BF16).astype(F32)
        att = mm(weights, cache[m, 1].reshape(1024, 128)) + new_weight * new[m, 1].astype(F32)
        proj = mm(att.astype(BF16), sout[m])
        for e in range(8):
            pbuf[e, m] = proj[:, e * 128 : (e + 1) * 128]
    with jax.named_scope("barrier"):
        pl.semaphore_wait(barrier, 22)

    def to_x(kx):
        return (dp_at(0, kx), mp)

    def to_z(kz):
        return (dp_at(kz, 0), mp)

    def spread(buf, base, pa, pb):
        for k in (1, 3, 2):
            send(buf(0, 0, 0, 0), buf(0, 0, 0, k), base + k, to_x(k))
            send(buf(1, 0, 0, 0), buf(1, 0, k, 0), base + 3 + k, to_z(k))
        for k in (1, 3, 2):
            send(buf(0, 0, 0, 0), buf(0, 0, k, 0), pa, to_z(k))
            send(buf(1, 0, 0, 0), buf(1, 0, 0, k), pb, to_x(k))

    def forward(buf, base, pa, pb):
        for k in (1, 3, 2):
            wait_in(buf(0, k, 0, 0), base + k)
            for kz in (1, 3, 2):
                send(buf(0, k, 0, 0), buf(0, k, kz, 0), pa, to_z(kz))
            wait_in(buf(1, 4 * k, 0, 0), base + 3 + k)
            for kx in (1, 3, 2):
                send(buf(1, 4 * k, 0, 0), buf(1, 4 * k, 0, kx), pb, to_x(kx))
            sent(buf(0, 0, 0, 0), base + k)
            sent(buf(0, 0, 0, 0), base + 3 + k)

    def xblock(colour, place, az, ax):
        return xr.at[colour, place + 4 * az + ax]

    def sblock(colour, place, az, ax):
        return sall.at[c, colour, dp_at(4 - place // 4, 4 - place % 4)]

    spread(xblock, X1, XA, XB)
    sent(xr.at[0, pl.ds(0, 12)], XA)
    sent(xr.at[1, pl.ds(0, 12)], XB)

    for k, dev in enumerate(mp_peers):
        send(pbuf.at[dev[1]], prec.at[k], PR, dev)
    sent(prec, PR)

    forward(xblock, X1, XA, XB)

    need(router)
    logits = nt(normed, router[...])
    experts = iota((16, 8), 1).astype(F32)
    r0 = jnp.sum(jnp.where(own, rt0.astype(F32), 0.0), axis=1, keepdims=True)
    r1 = jnp.sum(jnp.where(own, rt1.astype(F32), 0.0), axis=1, keepdims=True)
    p0 = jnp.sum(jnp.where(experts == r0, logits, 0.0), axis=1, keepdims=True)
    p1 = jnp.sum(jnp.where(experts == r1, logits, 0.0), axis=1, keepdims=True)
    gate0 = 1.0 / (1.0 + jnp.exp(p1 - p0))
    gate1 = 1.0 / (1.0 + jnp.exp(p0 - p1))
    gs[0:1] = to_row(gate0, 128)
    gs[1:2] = to_row(gate1, 128)
    gr[dp] = gs[...]
    for dev in dp_peers:
        send(gs, gr.at[dp], G, dev)
    sent(gr.at[pl.ds(0, 15)], G)
    mine = mp.astype(F32)
    gate = jnp.where(r0 == mine, gate0, 0.0) + jnp.where(r1 == mine, gate1, 0.0)
    comb_s[...] = jnp.where(rank == iota((16, 128), 1).astype(F32), gate, 0.0)

    need(hidden, sgain)
    wait_in(prec, PR)
    head_cols = pl.ds(pl.multiple_of(mp * 128, 128), 128)
    state = hidden[:, :, head_cols].astype(F32) + pbuf[mp]
    for k in range(7):
        state = state + prec[k]
    stbuf[mp] = state
    for dev in mp_peers:
        send(stbuf.at[mp], stbuf.at[mp], ST, dev)
    sent(stbuf.at[pl.ds(0, 7)], ST)
    wait_in(stbuf.at[pl.ds(0, 7)], ST)
    sq_sum = jnp.zeros((16, 1), F32)
    for e in range(8):
        part = stbuf[e, c]
        sq_sum = sq_sum + jnp.sum(part * part, axis=1, keepdims=True)
    inv = lax.rsqrt(sq_sum * (1.0 / 1024.0) + EPS)
    both = sgain[...]
    g = jnp.where(c == 0, both[0:1], both[1:2])
    for e in range(8):
        cols = slice(e * 128, (e + 1) * 128)
        inner = slice(e % 4 * 128, (e % 4 + 1) * 128)
        sall[c, e // 4, dp, :, inner] = (stbuf[e, c] * inv * g[:, cols]).astype(BF16)
    need(bhead)
    for yy in range(4):
        rows = pl.ds(pl.multiple_of((2 * yy + 1 - c) * 512, 512), 512)
        send(bhead.at[rows], bhs.at[yy], HD, sibling)
    sent(bhs, HD)

    wait_in(xr.at[0, pl.ds(0, 12)], XA)
    wait_in(xr.at[1, pl.ds(0, 12)], XB)
    spread(sblock, Y1, SA, SB)
    sent(sall.at[0, 0, pl.ds(0, 12)], SA)
    sent(sall.at[0, 1, pl.ds(0, 12)], SB)
    with jax.named_scope("weights"):
        for cp in wcopies:
            cp.wait()

    def up_tile(col, width):
        cols = pl.ds(col, width)
        lo, hi = xr[0].reshape(128, half), xr[1].reshape(128, half)
        g = mm(lo, w_gate[:half, cols]) + mm(hi, w_gate[half:, cols])
        u = mm(lo, w_up[:half, cols]) + mm(hi, w_up[half:, cols])
        act[:, pl.ds(col, width)] = (g / (1.0 + jnp.exp(-g)) * u).astype(BF16)

    ff = w_gate.shape[1]
    full = ff // 256

    def up_body(i, carry):
        up_tile(pl.multiple_of(i * 256, 256), 256)
        return carry

    lax.fori_loop(0, full, up_body, 0)
    if ff % 256:
        up_tile(full * 256, ff % 256)

    forward(sblock, Y1, SA, SB)
    need(w_down)
    for core in range(2):
        phase = R1 if core == 0 else Y1 + 7
        for k in (2, 1, 3, 0):
            to_y = lax.rem(y + k, 4)
            owner = 2 * to_y + core
            res = mm(act[...], w_down[:, pl.ds(pl.multiple_of(owner * 512, 512), 512)])
            inner = pl.ds(pl.multiple_of(to_y * 256, 256), 256)
            r1s[core, :, :, inner] = res[:, :256].reshape(16, 8, 256).astype(BF16)
            second = res[:, 256:].astype(BF16)
            r2s[core, k] = second
            if k:
                send(r2s.at[core, k], r2r.at[mp], R2, (dp, owner))
            else:

                @pl.when(c != core)
                def _():
                    send(r2s.at[core, 0], r2r.at[mp], R2, (dp, owner))

                @pl.when(c == core)
                def _():
                    r2r[mp] = second

        for k in (1, 3, 4, 12, 5, 7, 13, 15, 2, 8, 6, 14, 9, 11, 10):
            send(r1s.at[core, k], r1r.at[core, k], phase, (dp_at(4 - k // 4, 4 - k % 4), mp))
        sent(r1r.at[0, pl.ds(0, 15)], phase)
    sent(r2r.at[pl.ds(0, 7)], R2)

    wait_in(gr.at[pl.ds(0, 15)], G)

    def spread_rows(rows):
        diag = iota((16, 16, 128), 1) == iota((16, 16, 128), 2)
        return jnp.sum(jnp.where(diag, rows, 0.0), axis=2, keepdims=True).reshape(256, 1)

    route0, route1 = to_col(rt0.astype(F32), 256), to_col(rt1.astype(F32), 256)
    lane = iota((256, 128), 1)
    named0, named1 = lane.astype(F32) == route0, lane.astype(F32) == route1
    t_row, t_col = iota((256, 256), 0), iota((256, 256), 1)
    before = ((t_row >> 4) == (t_col >> 4)) & (t_col < t_row)
    ranks = mm(
        jnp.where(before, 1.0, 0.0).astype(BF16), jnp.where(named0 | named1, 1.0, 0.0).astype(BF16)
    )
    gates = jnp.where(named0, spread_rows(gr[:, 0:1, :]), 0.0) + jnp.where(
        named1, spread_rows(gr[:, 1:2, :]), 0.0
    )
    block = ((z + 4 - (lane >> 5)) & 3) * 4 + ((x + 4 - ((lane >> 3) & 3)) & 3)
    same = (iota((256, 128), 0) >> 4) == block
    slot = (lane & 7).astype(F32)
    for e in range(8):
        w = jnp.where(same & (ranks[:, e : e + 1] == slot), gates[:, e : e + 1], 0.0)
        high = w.astype(BF16)
        wh[:, e * 128 : (e + 1) * 128] = high
        wl[:, e * 128 : (e + 1) * 128] = (w - high.astype(F32)).astype(BF16)

    wait_in(sall.at[0, 0, pl.ds(0, 12)], SA)
    wait_in(sall.at[0, 1, pl.ds(0, 12)], SB)
    send(sall.at[c], sall.at[c], S3, sibling)
    sent(sall.at[0], S3)
    need(shead)
    wait_in(sall.at[0], S3)
    for m in range(2):
        head = shead[:, m, :]
        part = nt(sall[m, 0].reshape(256, 512), head[:, :512]) + nt(
            sall[m, 1].reshape(256, 512), head[:, 512:]
        )
        slog[...] = part if m == 0 else ALPHA * (slog[...] - part)

    need(final_gain)

    def over_dp(buf, phase):
        for dev in dp_peers:
            send(buf, buf, phase, dev)

    comb = comb_s[...]

    def mix(core):
        phase = R1 if core == 0 else Y1 + 7
        wait_in(r1r.at[core, pl.ds(1, 15)], phase)
        total = r1s[core, 0].astype(F32)
        for k in range(1, 16):
            total = total + r1r[core, k].astype(F32)
        mixed = comb[:, 0:1] * total[0:1, :]
        for s in range(1, 8):
            mixed = mixed + comb[:, s : s + 1] * total[s : s + 1, :]
        m1s[core] = mixed.astype(BF16)
        for k in range(4):
            dev = (dp, 2 * lax.rem(y + k, 4) + core)
            if k:
                send(m1s.at[core], m1r.at[mp], M1, dev)
            else:

                @pl.when(c != core)
                def _():
                    send(m1s.at[core], m1r.at[mp], M1, dev)

    mix(0)
    wait_in(r2r.at[pl.ds(0, 7)], R2)
    rows = r2r[...].reshape(1024, 256)
    d2s[...] = (mm(wh[...], rows) + mm(wl[...], rows)).astype(BF16).reshape(16, 16, 256)
    for k, dev in enumerate(dp_peers):
        send(d2s.at[dev[0]], d2r.at[k], D2, dev)
    sent(d2r, D2)
    mix(1)
    sent(m1r.at[pl.ds(0, 7)], M1)
    m1r[mp] = m1s[c]

    wait_in(d2r, D2)
    cols = pl.ds(pl.multiple_of(mp * 512 + 256, 256), 256)
    state = tokens[:, cols].astype(F32) + d2s[dp].astype(F32)
    for k in range(15):
        state = state + d2r[k].astype(F32)
    xb[y, dp] = (state * final_gain[:, cols]).astype(BF16)
    over_dp(xb.at[y, dp], B1)
    sent(xb.at[0, pl.ds(0, 15)], B1)
    square = jnp.sum(state * state, axis=1, keepdims=True)

    wait_in(m1r.at[pl.ds(0, 7)], M1)
    square1 = jnp.zeros((16, 1), F32)
    for yy in range(4):
        cols = pl.ds(pl.multiple_of((2 * yy + c) * 512, 256), 256)
        inner = slice(yy * 256, (yy + 1) * 256)
        state = tokens[:, cols].astype(F32)
        for e in range(8):
            state = state + m1r[e, :, inner].astype(F32)
        xa[dp, :, inner] = (state * final_gain[:, cols]).astype(BF16)
        square1 = square1 + jnp.sum(state * state, axis=1, keepdims=True)
    over_dp(xa.at[dp], A2)
    sent(xa.at[pl.ds(0, 15)], A2)
    sqs[...] = to_row(square + jnp.where(y == 0, square1, 0.0), 128)
    for k, dev in enumerate(mp_peers):
        send(sqs, sq1.at[k], Q1, dev)
    sent(sq1, Q1)
    wait_in(xb.at[0, pl.ds(0, 15)], B1)
    for dev in y_peers:
        send(xb.at[y], xb.at[y], B2, dev)
    sent(xb.at[pl.ds(0, 3)], B2)
    wait_in(sq1, Q1)
    total = sqs[...]
    for k in range(7):
        total = total + sq1[k]
    sq2[dp] = total
    over_dp(sq2.at[dp], Q2)
    sent(sq2.at[pl.ds(0, 15)], Q2)

    need(temp)
    temp_col = to_col(temp[...], 256)
    wait_in(bhs, HD)

    def own_rows(yy, at, size):
        return bhead[pl.ds(pl.multiple_of((2 * yy + c) * 512 + at, 256), size), :]

    def gathered(first, buf_rows, at):
        for yy in range(4):
            rows = buf_rows(yy)
            theirs, ours = mm(rows, bhs[yy, at : at + 256, :]), mm(rows, own_rows(yy, at, 256))
            fresh = first and yy == 0
            psib[...] = theirs if fresh else psib[...] + theirs
            pown[...] = ours if fresh else pown[...] + ours

    wait_in(xa.at[pl.ds(0, 15)], A2)
    gathered(True, lambda yy: xa[:, :, yy * 256 : (yy + 1) * 256].reshape(256, 256), 0)
    wait_in(xb.at[pl.ds(0, 3)], B2)
    gathered(False, lambda yy: xb[yy].reshape(256, 256), 256)
    send(psib, prcv, PX, sibling)
    sent(psib, PX)
    acc = pown[...]
    wait_in(sq2.at[pl.ds(0, 15)], Q2)
    sums = spread_rows(sq2[...])
    row_scale = lax.rsqrt(sums * (1.0 / 4096.0) + EPS)
    wait_in(prcv, PX)
    combined = temp_col * ((acc + prcv[...]) * row_scale + slog[...])
    peak = jnp.max(combined, axis=1, keepdims=True)
    lse = peak + jnp.log(jnp.sum(jnp.exp(combined - peak), axis=1, keepdims=True))

    def merge(first, buf, count):
        top = first
        for k in range(count):
            top = jnp.maximum(top, buf[k])
        out = jnp.exp(first - top)
        for k in range(count):
            out = out + jnp.exp(buf[k] - top)
        return top + jnp.log(out)

    row = to_row(lse, 256)
    lsend[0] = row
    for k, dev in enumerate(dp_peers):
        send(lsend.at[0], l1.at[k], L1, dev)
    sent(l1, L1)
    wait_in(l1, L1)
    row = merge(row, l1, 15)
    lsend[1] = row
    for k, dev in enumerate(mp_peers):
        send(lsend.at[1], l2.at[k], L2, dev)
    sent(l2, L2)
    wait_in(l2, L2)
    out_ref[...] = combined - to_col(merge(row, l2, 7), 256)

    for ref, phase in pending:
        rcopy(ref, ref, phase, sibling).wait_send()


def per_device(
    tokens, norm_gain, router, w_gate, w_up, w_down, final_gain, routes, steer_hidden,
    steer_query, steer_cache, steer_new, cache_len, steer_out, steer_gain, base_head,
    steer_head, inv_temp,
):
    args = (
        tokens, norm_gain.reshape(1, -1), router.T, w_gate, w_up, w_down,
        final_gain.reshape(1, -1), routes.T, steer_hidden, steer_query, steer_cache, steer_new,
        cache_len.reshape(1, -1), steer_out, steer_gain, base_head,
        jnp.transpose(steer_head, (2, 0, 1)), inv_temp.reshape(1, -1),
    )
    d = tokens.shape[1]
    vs = base_head.shape[1]

    def like(a, drop=0):
        return pltpu.VMEM(a.shape[drop:], a.dtype)

    fetched = [like(a, 1 if k in (3, 4, 5) else 0) for k, a in enumerate(args)]
    scratch = fetched + [
        pltpu.VMEM((2, 16, 8, d // 2), BF16),
        pltpu.VMEM((128, w_gate.shape[2]), BF16),
        pltpu.VMEM((8, 2, 16, 128), F32),
        pltpu.VMEM((7, 2, 16, 128), F32),
        pltpu.VMEM((8, 2, 16, 128), F32),
        pltpu.VMEM((2, 2, 16, 16, 512), BF16),
        pltpu.VMEM((2, 16, 8, 1024), BF16),
        pltpu.VMEM((2, 16, 8, 1024), BF16),
        pltpu.VMEM((2, 4, 128, 256), BF16),
        pltpu.VMEM((8, 128, 256), BF16),
        pltpu.VMEM((2, 16, 1024), BF16),
        pltpu.VMEM((8, 16, 1024), BF16),
        pltpu.VMEM((16, 16, 256), BF16),
        pltpu.VMEM((15, 16, 256), BF16),
        pltpu.VMEM((2, 128), F32),
        pltpu.VMEM((16, 2, 128), F32),
        pltpu.VMEM((256, 1024), BF16),
        pltpu.VMEM((256, 1024), BF16),
        pltpu.VMEM((16, 16, 1024), BF16),
        pltpu.VMEM((4, 16, 16, 256), BF16),
        pltpu.VMEM((4, 512, vs), BF16),
        pltpu.VMEM((256, vs), F32),
        pltpu.VMEM((256, vs), F32),
        pltpu.VMEM((256, vs), F32),
        pltpu.VMEM((7, 1, 128), F32),
        pltpu.VMEM((16, 1, 128), F32),
        pltpu.VMEM((1, 128), F32),
        pltpu.VMEM((2, 1, 256), F32),
        pltpu.VMEM((15, 1, 256), F32),
        pltpu.VMEM((7, 1, 256), F32),
        pltpu.VMEM((256, vs), F32),
        pltpu.VMEM((16, 128), F32),
        pltpu.SemaphoreType.DMA((13 + 2 * WC + 3,)),
        pltpu.SemaphoreType.DMA((35,)),
        pltpu.SemaphoreType.DMA((35,)),
    ]
    return pl.pallas_call(
        kernel,
        name="decode_step",
        out_shape=jax.ShapeDtypeStruct((256, vs), F32),
        in_specs=[pl.BlockSpec(memory_space=pltpu.HBM)] * len(args),
        out_specs=pl.BlockSpec(memory_space=pltpu.VMEM),
        scratch_shapes=scratch,
        compiler_params=pltpu.CompilerParams(
            collective_id=0, has_side_effects=True, vmem_limit_bytes=44 * 1024 * 1024
        ),
    )(*[pltpu.with_memory_space_constraint(a, pltpu.HBM) for a in args])


def solution(mesh):
    placed = (
        P("dp", None),
        P(),
        P(),
        P("mp", None, "dp"),
        P("mp", None, "dp"),
        P("mp", "dp", None),
        P(),
        P(),
        P(None, "dp", None),
        P(None, "dp", "mp"),
        P(None, None, "dp", None, "mp"),
        P(None, None, "dp", "mp"),
        P("dp"),
        P(None, "mp", None),
        P(),
        P(None, ("dp", "mp")),
        P(None, None, ("dp", "mp")),
        P(),
    )
    return jax.shard_map(
        per_device, mesh=mesh, in_specs=placed, out_specs=P(None, ("dp", "mp")), check_vma=False
    )
```

```python
import functools
import math

import jax
import jax.numpy as jnp
from jax import lax
from jax.experimental import pallas as pl
from jax.experimental.pallas import tpu as pltpu
from jax.sharding import PartitionSpec as P

F32 = jnp.float32
BF16 = jnp.bfloat16
EPS = 1e-5
ALPHA = 2.0
HEAD_DIM = 128
WC = 4


def iota(shape, dim):
    return lax.broadcasted_iota(jnp.int32, shape, dim)


def eye(rows, cols):
    return iota((rows, cols), 0) == iota((rows, cols), 1)


def to_col(row, rows):
    if rows > 128:
        parts = [to_col(row[:, i : i + 128], 128) for i in range(0, rows, 128)]
        return jnp.concatenate(parts, axis=0)
    n = row.shape[1]
    return jnp.sum(jnp.where(eye(rows, n), row, 0.0), axis=1, keepdims=True)


def to_row(col, cols):
    if cols > 128:
        parts = [to_row(col[i : i + 128], 128) for i in range(0, cols, 128)]
        return jnp.concatenate(parts, axis=1)
    n = col.shape[0]
    return jnp.sum(jnp.where(eye(n, cols), col, 0.0), axis=0, keepdims=True)


def nt(a, b):
    return lax.dot_general(a, b, (((1,), (1,)), ((), ())), preferred_element_type=F32)


def mm(a, b):
    return jnp.dot(a, b, preferred_element_type=F32)


def kernel(
    tokens_h, norm_gain_h, router_h, w_gate_h, w_up_h, w_down_h, final_gain_h, routes_h,
    hidden_h, query_h, cache_h, new_h, len_h, sout_h, sgain_h, bhead_h, shead_h, temp_h,
    out_ref,
    tokens, norm_gain, router, w_gate, w_up, w_down, final_gain, routes,
    hidden, query, cache, new, clen, sout, sgain, shead, temp,
    xr, gpart, upart, act, pbuf, prec, stbuf, sall, r1s, r1r, r2s, r2r, m1s, m1r, d2s, d2r, gs, gr, wh, wl,
    xa, xb, bho, bht, bhs, psib, prcv, pown, sq1, sq2, sqs, lsend, l1, l2, slog, comb_s,
    lsem, bsem_s, bsem_r,
):
    dp = lax.axis_index("dp")
    mp = lax.axis_index("mp")
    y, c = mp // 2, mp % 2
    z, x = dp // 4, dp % 4

    zs = [z] + [lax.rem(z + k, 4) for k in (1, 2, 3)]
    xs = [x] + [lax.rem(x + k, 4) for k in (1, 2, 3)]

    def dp_at(kz, kx):
        return zs[kz % 4] * 4 + xs[kx % 4]

    dp_peers = [
        (dp_at(k // 4, k % 4), mp) for k in (1, 3, 4, 12, 5, 7, 13, 15, 2, 8, 6, 14, 9, 11, 10)
    ]
    def to_x(kx):
        return (dp_at(0, kx), mp)

    def to_z(kz):
        return (dp_at(kz, 0), mp)

    mp_peers = [(dp, lax.rem(mp + k, 8)) for k in range(1, 8)]
    y_peers = [(dp, lax.rem(y + k, 4) * 2 + c) for k in (1, 3, 2)]
    sibling = (dp, y * 2 + 1 - c)

    def rcopy(src, dst, phase, dev):
        return pltpu.make_async_remote_copy(
            src_ref=src, dst_ref=dst, send_sem=bsem_s.at[phase], recv_sem=bsem_r.at[phase],
            device_id=dev, device_id_type=pl.DeviceIdType.MESH,
        )

    pending = []

    def send(src, dst, phase, dev):
        rcopy(src, dst, phase, dev).start()

    def wait_in(ref, phase):
        with jax.named_scope("wait%d" % phase):
            rcopy(ref, ref, phase, sibling).wait_recv()

    def sent(ref, phase):
        pending.append((ref, phase))

    (XC, XD, X2) = (38, 39, 39)
    (XA, XB, PR, ST, SA, SB, S3, A2, B2, HD, PX, Q1, Q2, L1, L2, G, M1, D2, R2, R1) = range(20)
    X1, Y1, B1 = 20, 26, 34

    barrier = pltpu.get_barrier_semaphore()
    greeted = [to_x(k) for k in (1, 3, 2)] + [to_z(k) for k in (1, 3, 2)] + mp_peers
    for dev in greeted:
        pl.semaphore_signal(barrier, inc=1, device_id=dev, device_id_type=pl.DeviceIdType.MESH)

    pairs = [
        (tokens_h, tokens), (norm_gain_h, norm_gain), (routes_h, routes), (router_h, router),
        (query_h, query), (cache_h, cache), (new_h, new), (len_h, clen), (sout_h, sout),
        (hidden_h, hidden), (sgain_h, sgain),
        (final_gain_h, final_gain), (temp_h, temp),
    ]
    late = [(w_down_h.at[0], w_down), (shead_h, shead)]
    copies = {}

    def fetch(src, dst, n):
        cp = pltpu.make_async_copy(src, dst, lsem.at[n])
        cp.start()
        return cp

    n = 0
    for src, dst in pairs:
        copies[id(dst)] = fetch(src, dst, n)
        n += 1
    wcopies = []
    kw = w_gate.shape[0] // WC
    for i in range(WC):
        rows = pl.ds(i * kw, kw)
        wcopies.append(fetch(w_gate_h.at[0, rows], w_gate.at[rows], n))
        wcopies.append(fetch(w_up_h.at[0, rows], w_up.at[rows], n + 1))
        n += 2
    for src, dst in late:
        copies[id(dst)] = fetch(src, dst, n)
        n += 1

    for parity, dst in ((c, bho), (1 - c, bht)):
        for yy in range(4):
            for at in range(2):
                rows = pl.ds(pl.multiple_of((2 * yy + parity) * 512 + at * 256, 256), 256)
                pltpu.make_async_copy(
                    bhead_h.at[rows], dst.at[at, pl.ds(yy * 256, 256)],
                    lsem.at[n if dst is bho else n + 1],
                ).start()
    copies[id(bho)] = pltpu.make_async_copy(bho, bho, lsem.at[n])
    copies[id(bht)] = pltpu.make_async_copy(bht, bht, lsem.at[n + 1])

    def need(*refs):
        with jax.named_scope("need"):
            for r in refs:
                copies[id(r)].wait()

    need(tokens, norm_gain, routes)
    tok = tokens[...].astype(F32)
    mean_sq = jnp.mean(tok * tok, axis=1, keepdims=True)
    normed = (tok * lax.rsqrt(mean_sq + EPS) * norm_gain[...]).astype(BF16)
    rt = routes[...]
    lanes = iota((16, 256), 1)
    own = lanes == dp * 16 + iota((16, 256), 0)
    earlier = (lanes >= dp * 16) & (lanes < dp * 16 + iota((16, 256), 0))
    rt0, rt1 = rt[0:1, :], rt[1:2, :]

    def places(expert):
        hit_all = ((rt0 == expert) | (rt1 == expert)).astype(F32)
        hit = jnp.sum(jnp.where(own, hit_all, 0.0), axis=1, keepdims=True)
        rank = jnp.sum(jnp.where(earlier, hit_all, 0.0), axis=1, keepdims=True)
        return hit, rank

    hit, rank = places(mp)
    hit_row = jnp.sum(jnp.where(eye(16, 128), hit, 0.0), axis=0, keepdims=True)
    rank_row = jnp.sum(
        jnp.where(iota((16, 128), 0) < iota((16, 128), 1), hit, 0.0), axis=0, keepdims=True
    )
    select = jnp.where(
        (hit_row > 0.5) & (rank_row == iota((8, 128), 0).astype(F32)), 1.0, 0.0
    )[:, :16].astype(BF16)
    quarter = xr.shape[4]
    for colour in range(2):
        for chunk in range(2):
            at = (2 * colour + chunk) * quarter
            xr[chunk, colour, 0] = mm(select, normed[:, at : at + quarter]).astype(BF16)

    with jax.named_scope("barrier"):
        pl.semaphore_wait(barrier, len(greeted))

    def spread(buf, base, pa, pb):
        for k in (1, 3, 2):
            send(buf(0, 0, 0, 0), buf(0, 0, 0, k), base + k, to_x(k))
            send(buf(1, 0, 0, 0), buf(1, 0, k, 0), base + 3 + k, to_z(k))
        for k in (1, 3, 2):
            send(buf(0, 0, 0, 0), buf(0, 0, k, 0), pa, to_z(k))
            send(buf(1, 0, 0, 0), buf(1, 0, 0, k), pb, to_x(k))

    def forward(buf, base, pa, pb):
        for k in (1, 3, 2):
            wait_in(buf(0, k, 0, 0), base + k)
            for kz in (1, 3, 2):
                send(buf(0, k, 0, 0), buf(0, k, kz, 0), pa, to_z(kz))
            wait_in(buf(1, 4 * k, 0, 0), base + 3 + k)
            for kx in (1, 3, 2):
                send(buf(1, 4 * k, 0, 0), buf(1, 4 * k, 0, kx), pb, to_x(kx))
            sent(buf(0, 0, 0, 0), base + k)
            sent(buf(0, 0, 0, 0), base + 3 + k)

    def xblock0(colour, place, az, ax):
        return xr.at[0, colour, place + 4 * az + ax]

    def xblock1(colour, place, az, ax):
        return xr.at[1, colour, place + 4 * az + ax]

    def sblock(colour, place, az, ax):
        return sall.at[c, colour, dp_at(4 - place // 4, 4 - place % 4)]

    for block, base, pa, pb in ((xblock0, X1, XA, XB), (xblock1, X2, XC, XD)):
        spread(block, base, pa, pb)
        sent(xr.at[0, 0, pl.ds(0, 12)], pa)
        sent(xr.at[0, 0, pl.ds(0, 12)], pb)

    need(query, cache, new, clen, sout)
    len_col = to_col(clen[...].astype(F32), 16).astype(jnp.int32)
    pos = iota((16, 1024), 1) - 64 * iota((16, 1024), 0)
    live = (pos >= 0) & (pos < len_col)
    scale = 1.0 / math.sqrt(HEAD_DIM)
    for m in range(2):
        q = query[m]
        scores = nt(q, cache[m, 0].reshape(1024, 128)) * scale
        new_score = (
            jnp.sum(q.astype(F32) * new[m, 0].astype(F32), axis=1, keepdims=True) * scale
        )
        masked = jnp.where(live, scores, -1e30)
        summit = jnp.maximum(jnp.max(masked, axis=1, keepdims=True), new_score)
        expo = jnp.where(live, jnp.exp(masked - summit), 0.0)
        new_expo = jnp.exp(new_score - summit)
        denom = jnp.sum(expo, axis=1, keepdims=True) + new_expo
        weights = (expo / denom).astype(BF16)
        new_weight = (new_expo / denom).astype(BF16).astype(F32)
        att = mm(weights, cache[m, 1].reshape(1024, 128)) + new_weight * new[m, 1].astype(F32)
        proj = mm(att.astype(BF16), sout[m])
        for e in range(8):
            pbuf[e, m] = proj[:, e * 128 : (e + 1) * 128]
    for k, dev in enumerate(mp_peers):
        send(pbuf.at[dev[1]], prec.at[k], PR, dev)
    sent(prec, PR)

    forward(xblock0, X1, XA, XB)
    forward(xblock1, X2, XC, XD)

    need(router)
    logits = nt(normed, router[...])
    experts = iota((16, 8), 1).astype(F32)
    r0 = jnp.sum(jnp.where(own, rt0.astype(F32), 0.0), axis=1, keepdims=True)
    r1 = jnp.sum(jnp.where(own, rt1.astype(F32), 0.0), axis=1, keepdims=True)
    p0 = jnp.sum(jnp.where(experts == r0, logits, 0.0), axis=1, keepdims=True)
    p1 = jnp.sum(jnp.where(experts == r1, logits, 0.0), axis=1, keepdims=True)
    gate0 = 1.0 / (1.0 + jnp.exp(p1 - p0))
    gate1 = 1.0 / (1.0 + jnp.exp(p0 - p1))
    gs[0:1] = to_row(gate0, 128)
    gs[1:2] = to_row(gate1, 128)
    gr[dp] = gs[...]
    for dev in dp_peers:
        send(gs, gr.at[dp], G, dev)
    sent(gr.at[pl.ds(0, 15)], G)
    mine = mp.astype(F32)
    gate = jnp.where(r0 == mine, gate0, 0.0) + jnp.where(r1 == mine, gate1, 0.0)
    comb_s[...] = jnp.where(rank == iota((16, 128), 1).astype(F32), gate, 0.0)

    need(hidden, sgain)
    wait_in(prec, PR)
    head_cols = pl.ds(pl.multiple_of(mp * 128, 128), 128)
    state = hidden[:, :, head_cols].astype(F32) + pbuf[mp]
    for k in range(7):
        state = state + prec[k]
    stbuf[mp] = state
    for dev in mp_peers:
        send(stbuf.at[mp], stbuf.at[mp], ST, dev)
    sent(stbuf.at[pl.ds(0, 7)], ST)
    with jax.named_scope("weights"):
        for cp in wcopies:
            cp.wait()

    def up_tile(chunk, col, width):
        cols = pl.ds(col, width)
        g = u = None
        for colour in range(2):
            rows = xr[chunk, colour].reshape(128, quarter)
            depth = pl.ds((2 * colour + chunk) * quarter, quarter)
            dg, du = mm(rows, w_gate[depth, cols]), mm(rows, w_up[depth, cols])
            g, u = (dg, du) if g is None else (g + dg, u + du)
        if chunk == 0:
            gpart[:, cols] = g
            upart[:, cols] = u
        else:
            g, u = g + gpart[:, cols], u + upart[:, cols]
            act[:, cols] = (g / (1.0 + jnp.exp(-g)) * u).astype(BF16)

    ff = w_gate.shape[1]
    full = ff // 256

    def up_chunk(chunk, pa, pb):
        wait_in(xr.at[0, 0, pl.ds(0, 12)], pa)
        wait_in(xr.at[0, 0, pl.ds(0, 12)], pb)

        def up_body(i, carry):
            up_tile(chunk, pl.multiple_of(i * 256, 256), 256)
            return carry

        lax.fori_loop(0, full, up_body, 0)
        if ff % 256:
            up_tile(chunk, full * 256, ff % 256)

    up_chunk(0, XA, XB)

    wait_in(stbuf.at[pl.ds(0, 7)], ST)
    sq_sum = jnp.zeros((16, 1), F32)
    for e in range(8):
        part = stbuf[e, c]
        sq_sum = sq_sum + jnp.sum(part * part, axis=1, keepdims=True)
    inv = lax.rsqrt(sq_sum * (1.0 / 1024.0) + EPS)
    both = sgain[...]
    g = jnp.where(c == 0, both[0:1], both[1:2])
    for e in range(8):
        cols = slice(e * 128, (e + 1) * 128)
        inner = slice(e % 4 * 128, (e % 4 + 1) * 128)
        sall[c, e // 4, dp, :, inner] = (stbuf[e, c] * inv * g[:, cols]).astype(BF16)
    need(bht)
    send(bht, bhs, HD, sibling)
    sent(bhs, HD)

    spread(sblock, Y1, SA, SB)
    sent(sall.at[0, 0, pl.ds(0, 12)], SA)
    sent(sall.at[0, 1, pl.ds(0, 12)], SB)
    up_chunk(1, XC, XD)

    need(w_down)
    for core in range(2):
        phase = R1 if core == 0 else Y1 + 7
        for k in (2, 1, 3, 0):
            to_y = lax.rem(y + k, 4)
            owner = 2 * to_y + core
            res = mm(act[...], w_down[:, pl.ds(pl.multiple_of(owner * 512, 512), 512)])
            inner = pl.ds(pl.multiple_of(to_y * 256, 256), 256)
            r1s[core, :, :, inner] = res[:, :256].reshape(16, 8, 256).astype(BF16)
            second = res[:, 256:].astype(BF16)
            r2s[core, k] = second
            if k:
                send(r2s.at[core, k], r2r.at[mp], R2, (dp, owner))
            else:

                @pl.when(c != core)
                def _():
                    send(r2s.at[core, 0], r2r.at[mp], R2, (dp, owner))

                @pl.when(c == core)
                def _():
                    r2r[mp] = second

        for k in (1, 3, 4, 12, 5, 7, 13, 15, 2, 8, 6, 14, 9, 11, 10):
            send(r1s.at[core, k], r1r.at[core, k], phase, (dp_at(4 - k // 4, 4 - k % 4), mp))
        sent(r1r.at[0, pl.ds(0, 15)], phase)
    sent(r2r.at[pl.ds(0, 7)], R2)

    wait_in(gr.at[pl.ds(0, 15)], G)

    def spread_rows(rows):
        diag = iota((16, 16, 128), 1) == iota((16, 16, 128), 2)
        return jnp.sum(jnp.where(diag, rows, 0.0), axis=2, keepdims=True).reshape(256, 1)

    route0, route1 = to_col(rt0.astype(F32), 256), to_col(rt1.astype(F32), 256)
    lane = iota((256, 128), 1)
    named0, named1 = lane.astype(F32) == route0, lane.astype(F32) == route1
    t_row, t_col = iota((256, 256), 0), iota((256, 256), 1)
    before = ((t_row >> 4) == (t_col >> 4)) & (t_col < t_row)
    ranks = mm(
        jnp.where(before, 1.0, 0.0).astype(BF16), jnp.where(named0 | named1, 1.0, 0.0).astype(BF16)
    )
    gates = jnp.where(named0, spread_rows(gr[:, 0:1, :]), 0.0) + jnp.where(
        named1, spread_rows(gr[:, 1:2, :]), 0.0
    )
    block = ((z + 4 - (lane >> 5)) & 3) * 4 + ((x + 4 - ((lane >> 3) & 3)) & 3)
    same = (iota((256, 128), 0) >> 4) == block
    slot = (lane & 7).astype(F32)
    for e in range(8):
        w = jnp.where(same & (ranks[:, e : e + 1] == slot), gates[:, e : e + 1], 0.0)
        high = w.astype(BF16)
        wh[:, e * 128 : (e + 1) * 128] = high
        wl[:, e * 128 : (e + 1) * 128] = (w - high.astype(F32)).astype(BF16)

    need(final_gain)

    def over_dp(buf, phase):
        for dev in dp_peers:
            send(buf, buf, phase, dev)

    comb = comb_s[...]

    def mix(core):
        phase = R1 if core == 0 else Y1 + 7
        wait_in(r1r.at[core, pl.ds(1, 15)], phase)
        total = r1s[core, 0].astype(F32)
        for k in range(1, 16):
            total = total + r1r[core, k].astype(F32)
        mixed = comb[:, 0:1] * total[0:1, :]
        for s in range(1, 8):
            mixed = mixed + comb[:, s : s + 1] * total[s : s + 1, :]
        m1s[core] = mixed.astype(BF16)
        for k in range(4):
            dev = (dp, 2 * lax.rem(y + k, 4) + core)
            if k:
                send(m1s.at[core], m1r.at[mp], M1, dev)
            else:

                @pl.when(c != core)
                def _():
                    send(m1s.at[core], m1r.at[mp], M1, dev)

    wait_in(r2r.at[pl.ds(0, 7)], R2)
    rows = r2r[...].reshape(1024, 256)
    d2s[...] = (mm(wh[...], rows) + mm(wl[...], rows)).astype(BF16).reshape(16, 16, 256)
    for k, dev in enumerate(dp_peers):
        send(d2s.at[dev[0]], d2r.at[k], D2, dev)
    sent(d2r, D2)
    forward(sblock, Y1, SA, SB)
    mix(0)
    mix(1)
    sent(m1r.at[pl.ds(0, 7)], M1)
    m1r[mp] = m1s[c]

    wait_in(d2r, D2)
    cols = pl.ds(pl.multiple_of(mp * 512 + 256, 256), 256)
    state = tokens[:, cols].astype(F32) + d2s[dp].astype(F32)
    for k in range(15):
        state = state + d2r[k].astype(F32)
    y_cols = pl.ds(pl.multiple_of(y * 256, 256), 256)
    xb[dp, :, y_cols] = (state * final_gain[:, cols]).astype(BF16)
    block = xb.at[dp, :, y_cols]
    for kz in range(4):
        for kx in (0, 1, 3, 2):
            if kz or kx:
                send(block, block, B1 + kz, (dp_at(kz, kx), mp))
        sent(xb.at[pl.ds(0, 4 if kz else 3), :, pl.ds(0, 256)], B1 + kz)
    square = jnp.sum(state * state, axis=1, keepdims=True)

    wait_in(m1r.at[pl.ds(0, 7)], M1)
    square1 = jnp.zeros((16, 1), F32)
    for yy in range(4):
        cols = pl.ds(pl.multiple_of((2 * yy + c) * 512, 256), 256)
        inner = slice(yy * 256, (yy + 1) * 256)
        state = tokens[:, cols].astype(F32)
        for e in range(8):
            state = state + m1r[e, :, inner].astype(F32)
        xa[dp, :, inner] = (state * final_gain[:, cols]).astype(BF16)
        square1 = square1 + jnp.sum(state * state, axis=1, keepdims=True)
    over_dp(xa.at[dp], A2)
    sent(xa.at[pl.ds(0, 15)], A2)
    sqs[...] = to_row(square + jnp.where(y == 0, square1, 0.0), 128)
    for k, dev in enumerate(mp_peers):
        send(sqs, sq1.at[k], Q1, dev)
    sent(sq1, Q1)

    def group(kz):
        wait_in(xb.at[pl.ds(0, 4 if kz else 3), :, pl.ds(0, 256)], B1 + kz)
        blocks = xb.at[pl.ds(4 * zs[(4 - kz) % 4], 4), :, y_cols]
        for dev in y_peers:
            send(blocks, blocks, B2, dev)

    wait_in(sall.at[0, 0, pl.ds(0, 12)], SA)
    wait_in(sall.at[0, 1, pl.ds(0, 12)], SB)
    send(sall.at[c], sall.at[c], S3, sibling)
    sent(sall.at[0], S3)

    group(0)
    wait_in(sq1, Q1)
    total = sqs[...]
    for k in range(7):
        total = total + sq1[k]
    sq2[dp] = total
    over_dp(sq2.at[dp], Q2)
    sent(sq2.at[pl.ds(0, 15)], Q2)
    group(1)
    group(3)
    group(2)
    sent(xb.at[:, :, pl.ds(0, 768)], B2)

    need(shead)
    wait_in(sall.at[0], S3)
    for m in range(2):
        head = shead[:, m, :]
        part = nt(sall[m, 0].reshape(256, 512), head[:, :512]) + nt(
            sall[m, 1].reshape(256, 512), head[:, 512:]
        )
        slog[...] = part if m == 0 else ALPHA * (slog[...] - part)

    need(temp, bho)
    temp_col = to_col(temp[...], 256)
    wait_in(bhs, HD)
    wait_in(xa.at[pl.ds(0, 15)], A2)
    rows = xa[...].reshape(256, 1024)
    psib[...] = mm(rows, bhs[0])
    pown[...] = mm(rows, bho[0])
    wait_in(xb.at[:, :, pl.ds(0, 768)], B2)
    rows = xb[...].reshape(256, 1024)
    psib[...] += mm(rows, bhs[1])
    send(psib, prcv, PX, sibling)
    sent(psib, PX)
    acc = pown[...] + mm(rows, bho[1])
    wait_in(sq2.at[pl.ds(0, 15)], Q2)
    sums = spread_rows(sq2[...])
    row_scale = lax.rsqrt(sums * (1.0 / 4096.0) + EPS)
    wait_in(prcv, PX)
    combined = temp_col * ((acc + prcv[...]) * row_scale + slog[...])
    peak = jnp.max(combined, axis=1, keepdims=True)
    lse = peak + jnp.log(jnp.sum(jnp.exp(combined - peak), axis=1, keepdims=True))

    def merge(first, buf, count):
        top = first
        for k in range(count):
            top = jnp.maximum(top, buf[k])
        out = jnp.exp(first - top)
        for k in range(count):
            out = out + jnp.exp(buf[k] - top)
        return top + jnp.log(out)

    row = to_row(lse, 256)
    lsend[0] = row
    for k, dev in enumerate(dp_peers):
        send(lsend.at[0], l1.at[k], L1, dev)
    sent(l1, L1)
    wait_in(l1, L1)
    row = merge(row, l1, 15)
    lsend[1] = row
    for k, dev in enumerate(mp_peers):
        send(lsend.at[1], l2.at[k], L2, dev)
    sent(l2, L2)
    for ref, phase in pending:
        rcopy(ref, ref, phase, sibling).wait_send()
    wait_in(l2, L2)
    out_ref[...] = combined - to_col(merge(row, l2, 7), 256)


def per_device(
    tokens, norm_gain, router, w_gate, w_up, w_down, final_gain, routes, steer_hidden,
    steer_query, steer_cache, steer_new, cache_len, steer_out, steer_gain, base_head,
    steer_head, inv_temp,
):
    args = (
        tokens, norm_gain.reshape(1, -1), router.T, w_gate, w_up, w_down,
        final_gain.reshape(1, -1), routes.T, steer_hidden, steer_query, steer_cache, steer_new,
        cache_len.reshape(1, -1), steer_out, steer_gain, base_head,
        jnp.transpose(steer_head, (2, 0, 1)), inv_temp.reshape(1, -1),
    )
    d = tokens.shape[1]
    vs = base_head.shape[1]

    def like(a, drop=0):
        return pltpu.VMEM(a.shape[drop:], a.dtype)

    fetched = [like(a, 1 if k in (3, 4, 5) else 0) for k, a in enumerate(args) if k != 15]
    scratch = fetched + [
        pltpu.VMEM((2, 2, 16, 8, d // 4), BF16),
        pltpu.VMEM((128, w_gate.shape[2]), F32),
        pltpu.VMEM((128, w_gate.shape[2]), F32),
        pltpu.VMEM((128, w_gate.shape[2]), BF16),
        pltpu.VMEM((8, 2, 16, 128), F32),
        pltpu.VMEM((7, 2, 16, 128), F32),
        pltpu.VMEM((8, 2, 16, 128), F32),
        pltpu.VMEM((2, 2, 16, 16, 512), BF16),
        pltpu.VMEM((2, 16, 8, 1024), BF16),
        pltpu.VMEM((2, 16, 8, 1024), BF16),
        pltpu.VMEM((2, 4, 128, 256), BF16),
        pltpu.VMEM((8, 128, 256), BF16),
        pltpu.VMEM((2, 16, 1024), BF16),
        pltpu.VMEM((8, 16, 1024), BF16),
        pltpu.VMEM((16, 16, 256), BF16),
        pltpu.VMEM((15, 16, 256), BF16),
        pltpu.VMEM((2, 128), F32),
        pltpu.VMEM((16, 2, 128), F32),
        pltpu.VMEM((256, 1024), BF16),
        pltpu.VMEM((256, 1024), BF16),
        pltpu.VMEM((16, 16, 1024), BF16),
        pltpu.VMEM((16, 16, 1024), BF16),
        pltpu.VMEM((2, 1024, vs), BF16),
        pltpu.VMEM((2, 1024, vs), BF16),
        pltpu.VMEM((2, 1024, vs), BF16),
        pltpu.VMEM((256, vs), F32),
        pltpu.VMEM((256, vs), F32),
        pltpu.VMEM((256, vs), F32),
        pltpu.VMEM((7, 1, 128), F32),
        pltpu.VMEM((16, 1, 128), F32),
        pltpu.VMEM((1, 128), F32),
        pltpu.VMEM((2, 1, 256), F32),
        pltpu.VMEM((15, 1, 256), F32),
        pltpu.VMEM((7, 1, 256), F32),
        pltpu.VMEM((256, vs), F32),
        pltpu.VMEM((16, 128), F32),
        pltpu.SemaphoreType.DMA((13 + 2 * WC + 4,)),
        pltpu.SemaphoreType.DMA((46,)),
        pltpu.SemaphoreType.DMA((46,)),
    ]
    return pl.pallas_call(
        kernel,
        name="decode_step",
        out_shape=jax.ShapeDtypeStruct((256, vs), F32),
        in_specs=[pl.BlockSpec(memory_space=pltpu.HBM)] * len(args),
        out_specs=pl.BlockSpec(memory_space=pltpu.VMEM),
        scratch_shapes=scratch,
        compiler_params=pltpu.CompilerParams(
            collective_id=0, has_side_effects=True, vmem_limit_bytes=44 * 1024 * 1024
        ),
    )(*[pltpu.with_memory_space_constraint(a, pltpu.HBM) for a in args])


def solution(mesh):
    placed = (
        P("dp", None),
        P(),
        P(),
        P("mp", None, "dp"),
        P("mp", None, "dp"),
        P("mp", "dp", None),
        P(),
        P(),
        P(None, "dp", None),
        P(None, "dp", "mp"),
        P(None, None, "dp", None, "mp"),
        P(None, None, "dp", "mp"),
        P("dp"),
        P(None, "mp", None),
        P(),
        P(None, ("dp", "mp")),
        P(None, None, ("dp", "mp")),
        P(),
    )
    return jax.shard_map(
        per_device, mesh=mesh, in_specs=placed, out_specs=P(None, ("dp", "mp")), check_vma=False
    )
```

```python
import functools
import math

import jax
import jax.numpy as jnp
from jax import lax
from jax.experimental import pallas as pl
from jax.experimental.pallas import tpu as pltpu
from jax.sharding import PartitionSpec as P

F32 = jnp.float32
BF16 = jnp.bfloat16
EPS = 1e-5
ALPHA = 2.0
HEAD_DIM = 128
WC = 4


def iota(shape, dim):
    return lax.broadcasted_iota(jnp.int32, shape, dim)


def eye(rows, cols):
    return iota((rows, cols), 0) == iota((rows, cols), 1)


def to_col(row, rows):
    if rows > 128:
        parts = [to_col(row[:, i : i + 128], 128) for i in range(0, rows, 128)]
        return jnp.concatenate(parts, axis=0)
    n = row.shape[1]
    return jnp.sum(jnp.where(eye(rows, n), row, 0.0), axis=1, keepdims=True)


def to_row(col, cols):
    if cols > 128:
        parts = [to_row(col[i : i + 128], 128) for i in range(0, cols, 128)]
        return jnp.concatenate(parts, axis=1)
    n = col.shape[0]
    return jnp.sum(jnp.where(eye(n, cols), col, 0.0), axis=0, keepdims=True)


def nt(a, b):
    return lax.dot_general(a, b, (((1,), (1,)), ((), ())), preferred_element_type=F32)


def mm(a, b):
    return jnp.dot(a, b, preferred_element_type=F32)


def kernel(
    tokens_h, norm_gain_h, router_h, w_gate_h, w_up_h, w_down_h, final_gain_h, routes_h,
    hidden_h, query_h, cache_h, new_h, len_h, sout_h, sgain_h, bhead_h, shead_h, temp_h,
    out_ref,
    tokens, norm_gain, router, w_gate, w_up, w_down, final_gain, routes,
    hidden, query, cache, new, clen, sout, sgain, shead, temp,
    xr, gpart, upart, act, pbuf, prec, stbuf, sall, r1s, r1r, r2s, r2r, m1s, m1r, d2s, d2r, gs, gr, wh, wl,
    xa, xb, bho, bht, bhs, psib, prcv, pown, sq1, sq2, sqs, lsend, l1, l2, slog, comb_s,
    lsem, bsem_s, bsem_r,
):
    dp = lax.axis_index("dp")
    mp = lax.axis_index("mp")
    y, c = mp // 2, mp % 2
    z, x = dp // 4, dp % 4

    zs = [z] + [lax.rem(z + k, 4) for k in (1, 2, 3)]
    xs = [x] + [lax.rem(x + k, 4) for k in (1, 2, 3)]

    def dp_at(kz, kx):
        return zs[kz % 4] * 4 + xs[kx % 4]

    dp_peers = [
        (dp_at(k // 4, k % 4), mp) for k in (10, 9, 11, 6, 14, 2, 8, 5, 7, 13, 15, 1, 3, 4, 12)
    ]
    def to_x(kx):
        return (dp_at(0, kx), mp)

    def to_z(kz):
        return (dp_at(kz, 0), mp)

    mp_peers = [(dp, lax.rem(mp + k, 8)) for k in (4, 3, 5, 2, 6, 1, 7)]
    y_peers = [(dp, lax.rem(y + k, 4) * 2 + c) for k in (2, 1, 3)]
    sibling = (dp, y * 2 + 1 - c)

    def rcopy(src, dst, phase, dev):
        return pltpu.make_async_remote_copy(
            src_ref=src, dst_ref=dst, send_sem=bsem_s.at[phase], recv_sem=bsem_r.at[phase],
            device_id=dev, device_id_type=pl.DeviceIdType.MESH,
        )

    pending = []

    def send(src, dst, phase, dev):
        rcopy(src, dst, phase, dev).start()

    def wait_in(ref, phase):
        with jax.named_scope("wait%d" % phase):
            rcopy(ref, ref, phase, sibling).wait_recv()

    def sent(ref, phase):
        pending.append((ref, phase))

    (XC, XD, X2) = (38, 39, 39)
    (XA, XB, PR, ST, SA, SB, S3, A2, B2, HD, PX, Q1, Q2, L1, L2, G, M1, D2, R2, R1) = range(20)
    X1, Y1, B1 = 20, 26, 34

    barrier = pltpu.get_barrier_semaphore()
    greeted = [to_x(k) for k in (1, 3, 2)] + [to_z(k) for k in (1, 3, 2)] + mp_peers
    for dev in greeted:
        pl.semaphore_signal(barrier, inc=1, device_id=dev, device_id_type=pl.DeviceIdType.MESH)

    pairs = [
        (tokens_h, tokens), (norm_gain_h, norm_gain), (routes_h, routes), (router_h, router),
        (query_h, query), (cache_h, cache), (new_h, new), (len_h, clen), (sout_h, sout),
        (hidden_h, hidden), (sgain_h, sgain),
        (final_gain_h, final_gain), (temp_h, temp),
    ]
    late = [(w_down_h.at[0], w_down), (shead_h, shead)]
    copies = {}

    def fetch(src, dst, n):
        cp = pltpu.make_async_copy(src, dst, lsem.at[n])
        cp.start()
        return cp

    n = 0
    for src, dst in pairs:
        copies[id(dst)] = fetch(src, dst, n)
        n += 1
    wcopies = []
    kw = w_gate.shape[0] // WC
    for i in range(WC):
        rows = pl.ds(i * kw, kw)
        wcopies.append(fetch(w_gate_h.at[0, rows], w_gate.at[rows], n))
        wcopies.append(fetch(w_up_h.at[0, rows], w_up.at[rows], n + 1))
        n += 2
    for src, dst in late:
        copies[id(dst)] = fetch(src, dst, n)
        n += 1

    for parity, dst in ((c, bho), (1 - c, bht)):
        for yy in range(4):
            for at in range(2):
                rows = pl.ds(pl.multiple_of((2 * yy + parity) * 512 + at * 256, 256), 256)
                pltpu.make_async_copy(
                    bhead_h.at[rows], dst.at[at, pl.ds(yy * 256, 256)],
                    lsem.at[n if dst is bho else n + 1],
                ).start()
    copies[id(bho)] = pltpu.make_async_copy(bho, bho, lsem.at[n])
    copies[id(bht)] = pltpu.make_async_copy(bht, bht, lsem.at[n + 1])

    def need(*refs):
        with jax.named_scope("need"):
            for r in refs:
                copies[id(r)].wait()

    need(tokens, norm_gain, routes)
    tok = tokens[...].astype(F32)
    mean_sq = jnp.mean(tok * tok, axis=1, keepdims=True)
    normed = (tok * lax.rsqrt(mean_sq + EPS) * norm_gain[...]).astype(BF16)
    rt = routes[...]
    lanes = iota((16, 256), 1)
    own = lanes == dp * 16 + iota((16, 256), 0)
    earlier = (lanes >= dp * 16) & (lanes < dp * 16 + iota((16, 256), 0))
    rt0, rt1 = rt[0:1, :], rt[1:2, :]

    def places(expert):
        hit_all = ((rt0 == expert) | (rt1 == expert)).astype(F32)
        hit = jnp.sum(jnp.where(own, hit_all, 0.0), axis=1, keepdims=True)
        rank = jnp.sum(jnp.where(earlier, hit_all, 0.0), axis=1, keepdims=True)
        return hit, rank

    hit, rank = places(mp)
    hit_row = jnp.sum(jnp.where(eye(16, 128), hit, 0.0), axis=0, keepdims=True)
    rank_row = jnp.sum(
        jnp.where(iota((16, 128), 0) < iota((16, 128), 1), hit, 0.0), axis=0, keepdims=True
    )
    select = jnp.where(
        (hit_row > 0.5) & (rank_row == iota((8, 128), 0).astype(F32)), 1.0, 0.0
    )[:, :16].astype(BF16)
    quarter = xr.shape[4]
    for colour in range(2):
        for chunk in range(2):
            at = (2 * colour + chunk) * quarter
            xr[chunk, colour, 0] = mm(select, normed[:, at : at + quarter]).astype(BF16)

    with jax.named_scope("barrier"):
        pl.semaphore_wait(barrier, len(greeted))

    def spread(buf, base, pa, pb):
        for k in (2, 1, 3):
            send(buf(0, 0, 0, 0), buf(0, 0, 0, k), base + k, to_x(k))
            send(buf(1, 0, 0, 0), buf(1, 0, k, 0), base + 3 + k, to_z(k))
        for k in (2, 1, 3):
            send(buf(0, 0, 0, 0), buf(0, 0, k, 0), pa, to_z(k))
            send(buf(1, 0, 0, 0), buf(1, 0, 0, k), pb, to_x(k))

    def forward(buf, base, pa, pb):
        for k in (1, 3, 2):
            wait_in(buf(0, k, 0, 0), base + k)
            for kz in (2, 1, 3):
                send(buf(0, k, 0, 0), buf(0, k, kz, 0), pa, to_z(kz))
            wait_in(buf(1, 4 * k, 0, 0), base + 3 + k)
            for kx in (2, 1, 3):
                send(buf(1, 4 * k, 0, 0), buf(1, 4 * k, 0, kx), pb, to_x(kx))
            sent(buf(0, 0, 0, 0), base + k)
            sent(buf(0, 0, 0, 0), base + 3 + k)

    def xblock0(colour, place, az, ax):
        return xr.at[0, colour, place + 4 * az + ax]

    def xblock1(colour, place, az, ax):
        return xr.at[1, colour, place + 4 * az + ax]

    def sblock(colour, place, az, ax):
        return sall.at[c, colour, dp_at(4 - place // 4, 4 - place % 4)]

    for block, base, pa, pb in ((xblock0, X1, XA, XB), (xblock1, X2, XC, XD)):
        spread(block, base, pa, pb)
        sent(xr.at[0, 0, pl.ds(0, 12)], pa)
        sent(xr.at[0, 0, pl.ds(0, 12)], pb)

    need(query, cache, new, clen, sout)
    len_col = to_col(clen[...].astype(F32), 16).astype(jnp.int32)
    pos = iota((16, 1024), 1) - 64 * iota((16, 1024), 0)
    live = (pos >= 0) & (pos < len_col)
    scale = 1.0 / math.sqrt(HEAD_DIM)
    for m in range(2):
        q = query[m]
        scores = nt(q, cache[m, 0].reshape(1024, 128)) * scale
        new_score = (
            jnp.sum(q.astype(F32) * new[m, 0].astype(F32), axis=1, keepdims=True) * scale
        )
        masked = jnp.where(live, scores, -1e30)
        summit = jnp.maximum(jnp.max(masked, axis=1, keepdims=True), new_score)
        expo = jnp.where(live, jnp.exp(masked - summit), 0.0)
        new_expo = jnp.exp(new_score - summit)
        denom = jnp.sum(expo, axis=1, keepdims=True) + new_expo
        weights = (expo / denom).astype(BF16)
        new_weight = (new_expo / denom).astype(BF16).astype(F32)
        att = mm(weights, cache[m, 1].reshape(1024, 128)) + new_weight * new[m, 1].astype(F32)
        proj = mm(att.astype(BF16), sout[m])
        for e in range(8):
            pbuf[e, m] = proj[:, e * 128 : (e + 1) * 128]
    for k, dev in enumerate(mp_peers):
        send(pbuf.at[dev[1]], prec.at[k], PR, dev)
    sent(prec, PR)

    forward(xblock0, X1, XA, XB)
    forward(xblock1, X2, XC, XD)

    need(router)
    logits = nt(normed, router[...])
    experts = iota((16, 8), 1).astype(F32)
    r0 = jnp.sum(jnp.where(own, rt0.astype(F32), 0.0), axis=1, keepdims=True)
    r1 = jnp.sum(jnp.where(own, rt1.astype(F32), 0.0), axis=1, keepdims=True)
    p0 = jnp.sum(jnp.where(experts == r0, logits, 0.0), axis=1, keepdims=True)
    p1 = jnp.sum(jnp.where(experts == r1, logits, 0.0), axis=1, keepdims=True)
    gate0 = 1.0 / (1.0 + jnp.exp(p1 - p0))
    gate1 = 1.0 / (1.0 + jnp.exp(p0 - p1))
    gs[0:1] = to_row(gate0, 128)
    gs[1:2] = to_row(gate1, 128)
    gr[dp] = gs[...]
    for dev in dp_peers:
        send(gs, gr.at[dp], G, dev)
    sent(gr.at[pl.ds(0, 15)], G)
    mine = mp.astype(F32)
    gate = jnp.where(r0 == mine, gate0, 0.0) + jnp.where(r1 == mine, gate1, 0.0)
    comb_s[...] = jnp.where(rank == iota((16, 128), 1).astype(F32), gate, 0.0)

    need(hidden, sgain)
    wait_in(prec, PR)
    head_cols = pl.ds(pl.multiple_of(mp * 128, 128), 128)
    state = hidden[:, :, head_cols].astype(F32) + pbuf[mp]
    for k in range(7):
        state = state + prec[k]
    stbuf[mp] = state
    for dev in mp_peers:
        send(stbuf.at[mp], stbuf.at[mp], ST, dev)
    sent(stbuf.at[pl.ds(0, 7)], ST)
    with jax.named_scope("weights"):
        for cp in wcopies:
            cp.wait()

    def up_tile(chunk, col, width):
        cols = pl.ds(col, width)
        g = u = None
        for colour in range(2):
            rows = xr[chunk, colour].reshape(128, quarter)
            depth = pl.ds((2 * colour + chunk) * quarter, quarter)
            dg, du = mm(rows, w_gate[depth, cols]), mm(rows, w_up[depth, cols])
            g, u = (dg, du) if g is None else (g + dg, u + du)
        if chunk == 0:
            gpart[:, cols] = g
            upart[:, cols] = u
        else:
            g, u = g + gpart[:, cols], u + upart[:, cols]
            act[:, cols] = (g / (1.0 + jnp.exp(-g)) * u).astype(BF16)

    ff = w_gate.shape[1]
    full = ff // 256

    def up_chunk(chunk, pa, pb):
        wait_in(xr.at[0, 0, pl.ds(0, 12)], pa)
        wait_in(xr.at[0, 0, pl.ds(0, 12)], pb)

        for i in range(full):
            up_tile(chunk, i * 256, 256)
        if ff % 256:
            up_tile(chunk, full * 256, ff % 256)

    up_chunk(0, XA, XB)

    wait_in(stbuf.at[pl.ds(0, 7)], ST)
    sq_sum = jnp.zeros((16, 1), F32)
    for e in range(8):
        part = stbuf[e, c]
        sq_sum = sq_sum + jnp.sum(part * part, axis=1, keepdims=True)
    inv = lax.rsqrt(sq_sum * (1.0 / 1024.0) + EPS)
    both = sgain[...]
    g = jnp.where(c == 0, both[0:1], both[1:2])
    for e in range(8):
        cols = slice(e * 128, (e + 1) * 128)
        inner = slice(e % 4 * 128, (e % 4 + 1) * 128)
        sall[c, e // 4, dp, :, inner] = (stbuf[e, c] * inv * g[:, cols]).astype(BF16)
    need(bht)
    send(bht, bhs, HD, sibling)
    sent(bhs, HD)

    spread(sblock, Y1, SA, SB)
    sent(sall.at[0, 0, pl.ds(0, 12)], SA)
    sent(sall.at[0, 1, pl.ds(0, 12)], SB)
    up_chunk(1, XC, XD)

    need(w_down)
    for core in range(2):
        phase = R1 if core == 0 else Y1 + 7
        for k in (2, 1, 3, 0):
            to_y = lax.rem(y + k, 4)
            owner = 2 * to_y + core
            res = mm(act[...], w_down[:, pl.ds(pl.multiple_of(owner * 512, 512), 512)])
            inner = pl.ds(pl.multiple_of(to_y * 256, 256), 256)
            r1s[core, :, :, inner] = res[:, :256].reshape(16, 8, 256).astype(BF16)
            second = res[:, 256:].astype(BF16)
            r2s[core, k] = second
            if k:
                send(r2s.at[core, k], r2r.at[mp], R2, (dp, owner))
            else:

                @pl.when(c != core)
                def _():
                    send(r2s.at[core, 0], r2r.at[mp], R2, (dp, owner))

                @pl.when(c == core)
                def _():
                    r2r[mp] = second

        for k in (10, 9, 11, 6, 14, 2, 8, 5, 7, 13, 15, 1, 3, 4, 12):
            send(r1s.at[core, k], r1r.at[core, k], phase, (dp_at(4 - k // 4, 4 - k % 4), mp))
        sent(r1r.at[0, pl.ds(0, 15)], phase)
    sent(r2r.at[pl.ds(0, 7)], R2)

    wait_in(gr.at[pl.ds(0, 15)], G)

    def spread_rows(rows):
        diag = iota((16, 16, 128), 1) == iota((16, 16, 128), 2)
        return jnp.sum(jnp.where(diag, rows, 0.0), axis=2, keepdims=True).reshape(256, 1)

    route0, route1 = to_col(rt0.astype(F32), 256), to_col(rt1.astype(F32), 256)
    lane = iota((256, 128), 1)
    named0, named1 = lane.astype(F32) == route0, lane.astype(F32) == route1
    t_row, t_col = iota((256, 256), 0), iota((256, 256), 1)
    before = ((t_row >> 4) == (t_col >> 4)) & (t_col < t_row)
    ranks = mm(
        jnp.where(before, 1.0, 0.0).astype(BF16), jnp.where(named0 | named1, 1.0, 0.0).astype(BF16)
    )
    gates = jnp.where(named0, spread_rows(gr[:, 0:1, :]), 0.0) + jnp.where(
        named1, spread_rows(gr[:, 1:2, :]), 0.0
    )
    block = ((z + 4 - (lane >> 5)) & 3) * 4 + ((x + 4 - ((lane >> 3) & 3)) & 3)
    same = (iota((256, 128), 0) >> 4) == block
    slot = (lane & 7).astype(F32)
    for e in range(8):
        w = jnp.where(same & (ranks[:, e : e + 1] == slot), gates[:, e : e + 1], 0.0)
        high = w.astype(BF16)
        wh[:, e * 128 : (e + 1) * 128] = high
        wl[:, e * 128 : (e + 1) * 128] = (w - high.astype(F32)).astype(BF16)

    need(final_gain)

    def over_dp(buf, phase):
        for dev in dp_peers:
            send(buf, buf, phase, dev)

    comb = comb_s[...]

    def mix(core):
        phase = R1 if core == 0 else Y1 + 7
        wait_in(r1r.at[core, pl.ds(1, 15)], phase)
        total = r1s[core, 0].astype(F32)
        for k in range(1, 16):
            total = total + r1r[core, k].astype(F32)
        mixed = comb[:, 0:1] * total[0:1, :]
        for s in range(1, 8):
            mixed = mixed + comb[:, s : s + 1] * total[s : s + 1, :]
        m1s[core] = mixed.astype(BF16)
        for k in range(4):
            dev = (dp, 2 * lax.rem(y + k, 4) + core)
            if k:
                send(m1s.at[core], m1r.at[mp], M1, dev)
            else:

                @pl.when(c != core)
                def _():
                    send(m1s.at[core], m1r.at[mp], M1, dev)

    wait_in(r2r.at[pl.ds(0, 7)], R2)
    rows = r2r[...].reshape(1024, 256)
    d2s[...] = (mm(wh[...], rows) + mm(wl[...], rows)).astype(BF16).reshape(16, 16, 256)
    for k, dev in enumerate(dp_peers):
        send(d2s.at[dev[0]], d2r.at[k], D2, dev)
    sent(d2r, D2)
    forward(sblock, Y1, SA, SB)
    mix(0)
    mix(1)
    sent(m1r.at[pl.ds(0, 7)], M1)
    m1r[mp] = m1s[c]

    wait_in(d2r, D2)
    cols = pl.ds(pl.multiple_of(mp * 512 + 256, 256), 256)
    state = tokens[:, cols].astype(F32) + d2s[dp].astype(F32)
    for k in range(15):
        state = state + d2r[k].astype(F32)
    y_cols = pl.ds(pl.multiple_of(y * 256, 256), 256)
    xb[dp, :, y_cols] = (state * final_gain[:, cols]).astype(BF16)
    block = xb.at[dp, :, y_cols]
    for kz in range(4):
        for kx in (0, 1, 3, 2):
            if kz or kx:
                send(block, block, B1 + kz, (dp_at(kz, kx), mp))
        sent(xb.at[pl.ds(0, 4 if kz else 3), :, pl.ds(0, 256)], B1 + kz)
    square = jnp.sum(state * state, axis=1, keepdims=True)

    wait_in(m1r.at[pl.ds(0, 7)], M1)
    square1 = jnp.zeros((16, 1), F32)
    for yy in range(4):
        cols = pl.ds(pl.multiple_of((2 * yy + c) * 512, 256), 256)
        inner = slice(yy * 256, (yy + 1) * 256)
        state = tokens[:, cols].astype(F32)
        for e in range(8):
            state = state + m1r[e, :, inner].astype(F32)
        xa[dp, :, inner] = (state * final_gain[:, cols]).astype(BF16)
        square1 = square1 + jnp.sum(state * state, axis=1, keepdims=True)
    over_dp(xa.at[dp], A2)
    sent(xa.at[pl.ds(0, 15)], A2)
    sqs[...] = to_row(square + jnp.where(y == 0, square1, 0.0), 128)
    for k, dev in enumerate(mp_peers):
        send(sqs, sq1.at[k], Q1, dev)
    sent(sq1, Q1)

    def group(kz):
        wait_in(xb.at[pl.ds(0, 4 if kz else 3), :, pl.ds(0, 256)], B1 + kz)
        blocks = xb.at[pl.ds(4 * zs[(4 - kz) % 4], 4), :, y_cols]
        for dev in y_peers:
            send(blocks, blocks, B2, dev)

    wait_in(sall.at[0, 0, pl.ds(0, 12)], SA)
    wait_in(sall.at[0, 1, pl.ds(0, 12)], SB)
    send(sall.at[c], sall.at[c], S3, sibling)
    sent(sall.at[0], S3)

    group(0)
    wait_in(sq1, Q1)
    total = sqs[...]
    for k in range(7):
        total = total + sq1[k]
    sq2[dp] = total
    over_dp(sq2.at[dp], Q2)
    sent(sq2.at[pl.ds(0, 15)], Q2)
    group(1)
    group(3)
    group(2)
    sent(xb.at[:, :, pl.ds(0, 768)], B2)

    need(shead)
    wait_in(sall.at[0], S3)
    for m in range(2):
        head = shead[:, m, :]
        part = nt(sall[m, 0].reshape(256, 512), head[:, :512]) + nt(
            sall[m, 1].reshape(256, 512), head[:, 512:]
        )
        slog[...] = part if m == 0 else ALPHA * (slog[...] - part)

    need(temp, bho)
    temp_col = to_col(temp[...], 256)
    wait_in(bhs, HD)
    wait_in(xa.at[pl.ds(0, 15)], A2)
    rows = xa[...].reshape(256, 1024)
    psib[...] = mm(rows, bhs[0])
    pown[...] = mm(rows, bho[0])
    wait_in(xb.at[:, :, pl.ds(0, 768)], B2)
    rows = xb[...].reshape(256, 1024)
    psib[...] += mm(rows, bhs[1])
    send(psib, prcv, PX, sibling)
    sent(psib, PX)
    acc = pown[...] + mm(rows, bho[1])
    wait_in(sq2.at[pl.ds(0, 15)], Q2)
    sums = spread_rows(sq2[...])
    row_scale = lax.rsqrt(sums * (1.0 / 4096.0) + EPS)
    wait_in(prcv, PX)
    combined = temp_col * ((acc + prcv[...]) * row_scale + slog[...])
    peak = jnp.max(combined, axis=1, keepdims=True)
    lse = peak + jnp.log(jnp.sum(jnp.exp(combined - peak), axis=1, keepdims=True))

    def merge(first, buf, count):
        top = first
        for k in range(count):
            top = jnp.maximum(top, buf[k])
        out = jnp.exp(first - top)
        for k in range(count):
            out = out + jnp.exp(buf[k] - top)
        return top + jnp.log(out)

    row = to_row(lse, 256)
    lsend[0] = row
    for k, dev in enumerate(dp_peers):
        send(lsend.at[0], l1.at[k], L1, dev)
    sent(l1, L1)
    wait_in(l1, L1)
    row = merge(row, l1, 15)
    lsend[1] = row
    for k, dev in enumerate(mp_peers):
        send(lsend.at[1], l2.at[k], L2, dev)
    sent(l2, L2)
    for ref, phase in pending:
        rcopy(ref, ref, phase, sibling).wait_send()
    wait_in(l2, L2)
    out_ref[...] = combined - to_col(merge(row, l2, 7), 256)


def per_device(
    tokens, norm_gain, router, w_gate, w_up, w_down, final_gain, routes, steer_hidden,
    steer_query, steer_cache, steer_new, cache_len, steer_out, steer_gain, base_head,
    steer_head, inv_temp,
):
    args = (
        tokens, norm_gain.reshape(1, -1), router.T, w_gate, w_up, w_down,
        final_gain.reshape(1, -1), routes.T, steer_hidden, steer_query, steer_cache, steer_new,
        cache_len.reshape(1, -1), steer_out, steer_gain, base_head,
        jnp.transpose(steer_head, (2, 0, 1)), inv_temp.reshape(1, -1),
    )
    d = tokens.shape[1]
    vs = base_head.shape[1]

    def like(a, drop=0):
        return pltpu.VMEM(a.shape[drop:], a.dtype)

    fetched = [like(a, 1 if k in (3, 4, 5) else 0) for k, a in enumerate(args) if k != 15]
    scratch = fetched + [
        pltpu.VMEM((2, 2, 16, 8, d // 4), BF16),
        pltpu.VMEM((128, w_gate.shape[2]), F32),
        pltpu.VMEM((128, w_gate.shape[2]), F32),
        pltpu.VMEM((128, w_gate.shape[2]), BF16),
        pltpu.VMEM((8, 2, 16, 128), F32),
        pltpu.VMEM((7, 2, 16, 128), F32),
        pltpu.VMEM((8, 2, 16, 128), F32),
        pltpu.VMEM((2, 2, 16, 16, 512), BF16),
        pltpu.VMEM((2, 16, 8, 1024), BF16),
        pltpu.VMEM((2, 16, 8, 1024), BF16),
        pltpu.VMEM((2, 4, 128, 256), BF16),
        pltpu.VMEM((8, 128, 256), BF16),
        pltpu.VMEM((2, 16, 1024), BF16),
        pltpu.VMEM((8, 16, 1024), BF16),
        pltpu.VMEM((16, 16, 256), BF16),
        pltpu.VMEM((15, 16, 256), BF16),
        pltpu.VMEM((2, 128), F32),
        pltpu.VMEM((16, 2, 128), F32),
        pltpu.VMEM((256, 1024), BF16),
        pltpu.VMEM((256, 1024), BF16),
        pltpu.VMEM((16, 16, 1024), BF16),
        pltpu.VMEM((16, 16, 1024), BF16),
        pltpu.VMEM((2, 1024, vs), BF16),
        pltpu.VMEM((2, 1024, vs), BF16),
        pltpu.VMEM((2, 1024, vs), BF16),
        pltpu.VMEM((256, vs), F32),
        pltpu.VMEM((256, vs), F32),
        pltpu.VMEM((256, vs), F32),
        pltpu.VMEM((7, 1, 128), F32),
        pltpu.VMEM((16, 1, 128), F32),
        pltpu.VMEM((1, 128), F32),
        pltpu.VMEM((2, 1, 256), F32),
        pltpu.VMEM((15, 1, 256), F32),
        pltpu.VMEM((7, 1, 256), F32),
        pltpu.VMEM((256, vs), F32),
        pltpu.VMEM((16, 128), F32),
        pltpu.SemaphoreType.DMA((13 + 2 * WC + 4,)),
        pltpu.SemaphoreType.DMA((46,)),
        pltpu.SemaphoreType.DMA((46,)),
    ]
    return pl.pallas_call(
        kernel,
        name="decode_step",
        out_shape=jax.ShapeDtypeStruct((256, vs), F32),
        in_specs=[pl.BlockSpec(memory_space=pltpu.HBM)] * len(args),
        out_specs=pl.BlockSpec(memory_space=pltpu.VMEM),
        scratch_shapes=scratch,
        compiler_params=pltpu.CompilerParams(
            collective_id=0, has_side_effects=True, vmem_limit_bytes=44 * 1024 * 1024
        ),
    )(*[pltpu.with_memory_space_constraint(a, pltpu.HBM) for a in args])


def solution(mesh):
    placed = (
        P("dp", None),
        P(),
        P(),
        P("mp", None, "dp"),
        P("mp", None, "dp"),
        P("mp", "dp", None),
        P(),
        P(),
        P(None, "dp", None),
        P(None, "dp", "mp"),
        P(None, None, "dp", None, "mp"),
        P(None, None, "dp", "mp"),
        P("dp"),
        P(None, "mp", None),
        P(),
        P(None, ("dp", "mp")),
        P(None, None, ("dp", "mp")),
        P(),
    )
    return jax.shard_map(
        per_device, mesh=mesh, in_specs=placed, out_specs=P(None, ("dp", "mp")), check_vma=False
    )
```
